256 devices in a mesh: gx: 8 (over y, core), gy: 8 (over x, z_hi), gz: 4 (over z_lo).
Axes of the slice: x: 4, y: 4, z: 8 (z_hi: 2, z_lo: 4; z = z_hi * 4 + z_lo), core: 2. Of those that a mesh axis runs over, the one named last changes fastest.
Arguments:
- rhs: float32 [3, 128, 256, 512], P(None, 'gx', 'gy', 'gz'), may hold values from -6 to 6
- viscous: float32 [8, 16, 32], P('gx', 'gy', 'gz'), may hold values from 0.3 to 3
- reaction: float32 [8, 16, 32], P('gx', 'gy', 'gz'), may hold values from 0.05 to 1
Outputs:
- correction: float32 [3, 128, 256, 512], P(None, 'gx', 'gy', 'gz')
The draws below stay inside these ranges and needn't reach their ends.
All inputs are finite; a program needn't handle non-finite values.
Results may differ from the reference program's by a relative error of at most 0.00008.
Values sent between devices are 32-bit elements; how exact they have to be, the bound alone decides.
A program may use at most 64 MiB of HBM per device.

```python
import math
import jax
import jax.numpy as jnp
from jax import lax

EDGE_POINTS = 16
COMP = 3
ELEMENTS_X = 8
ELEMENTS_Y = 16
ELEMENTS_Z = 32
NX = 128
NY = 256
NZ = 512


def levels(rng, extent, shards, smallest, high):
    gain = 1.0
    for dim, parts in shards:
        steps = jax.random.uniform(jax.random.fold_in(jax.random.fold_in(rng, 6), dim), (parts,), jnp.float32, smallest / len(shards), high / len(shards))
        gain = gain * jnp.repeat(jnp.exp(steps), extent[dim] // parts).reshape((-1,) + (1,) * (len(extent) - 1 - dim))
    return gain


def normal_values(key, extent, spread, limit, cuts=(), kind=jnp.bfloat16):
    drawn = spread * jax.random.normal(key, extent, jnp.float32)
    if cuts:
        drawn = drawn * levels(key, extent, cuts, -0.22, 0.18)
    return jnp.clip(drawn, -limit, limit).astype(kind)


def setup_inputs(seed: int = 0) -> dict:
    arg_keys = jax.random.split(jax.random.key(seed), 4)
    rhs = normal_values(arg_keys[0], (COMP, NX, NY, NZ), 1.0, 6.0, ((1, 8), (2, 8), (3, 4)), jnp.float32)
    viscous = jnp.clip(jnp.exp(math.log(3.0) - 2.3025851 * jax.random.uniform(arg_keys[1], (ELEMENTS_X, ELEMENTS_Y, ELEMENTS_Z), jnp.float32) ** levels(arg_keys[1], (ELEMENTS_X, ELEMENTS_Y, ELEMENTS_Z), ((0, 8), (1, 8), (2, 4)), -0.2, 0.2)), 0.3, 3.0)
    reaction = jnp.clip(jnp.exp(math.log(1.0) - 2.9957323 * jax.random.uniform(arg_keys[2], (ELEMENTS_X, ELEMENTS_Y, ELEMENTS_Z), jnp.float32) ** levels(arg_keys[2], (ELEMENTS_X, ELEMENTS_Y, ELEMENTS_Z), ((0, 8), (1, 8), (2, 4)), -0.2, 0.2)), 0.05, 1.0)
    return {"rhs": rhs, "viscous": viscous, "reaction": reaction}


highest = lax.Precision.HIGHEST

def tables():
    index = jnp.arange(EDGE_POINTS + 2).astype(jnp.float32)
    basis = jnp.sqrt(jnp.float32(2.0) / (EDGE_POINTS + 3)) * jnp.sin(jnp.pi * (index[:, None] + 1.0) * (index[None, :] + 1.0) / (EDGE_POINTS + 3))
    eigen_values = 2.0 - 2.0 * jnp.cos(jnp.pi * (index + 1.0) / (EDGE_POINTS + 3))
    return (basis, eigen_values)

def rear_part(values, axis, blocks):
    first_layer = lax.slice_in_dim(values, EDGE_POINTS, EDGE_POINTS * blocks + 1, stride=EDGE_POINTS, axis=axis)
    second_layer = lax.slice_in_dim(values, EDGE_POINTS + 1, EDGE_POINTS * blocks + 2, stride=EDGE_POINTS, axis=axis)
    return jnp.stack([first_layer, second_layer], axis=axis + 1)

def expand(field_values):
    spread_values = jnp.broadcast_to(field_values[:, None, :, None, :, None], (ELEMENTS_X, EDGE_POINTS, ELEMENTS_Y, EDGE_POINTS, ELEMENTS_Z, EDGE_POINTS))
    return spread_values.reshape(NX, NY, NZ)

def precondition(field, viscous, reaction):
    basis, eigen_values = tables()
    padded_field = jnp.pad(field, 1)
    span_along_x, span_along_y = (padded_field.shape[0], padded_field.shape[1])
    front_margin = padded_field[:, :, :EDGE_POINTS * ELEMENTS_Z].reshape(span_along_x, span_along_y, ELEMENTS_Z, EDGE_POINTS)
    rear_margin = rear_part(padded_field, 2, ELEMENTS_Z)
    eigen_modes = jnp.einsum('xyhp,pg->xyhg', front_margin, basis[:EDGE_POINTS], precision=highest) + jnp.einsum('xyhp,pg->xyhg', rear_margin, basis[EDGE_POINTS:], precision=highest)
    front_margin = eigen_modes[:, :EDGE_POINTS * ELEMENTS_Y].reshape(span_along_x, ELEMENTS_Y, EDGE_POINTS, ELEMENTS_Z, EDGE_POINTS + 2)
    rear_margin = rear_part(eigen_modes, 1, ELEMENTS_Y)
    eigen_modes = jnp.einsum('xfphg,pb->xfbhg', front_margin, basis[:EDGE_POINTS], precision=highest) + jnp.einsum('xfphg,pb->xfbhg', rear_margin, basis[EDGE_POINTS:], precision=highest)
    front_margin = eigen_modes[:EDGE_POINTS * ELEMENTS_X].reshape(ELEMENTS_X, EDGE_POINTS, ELEMENTS_Y, EDGE_POINTS + 2, ELEMENTS_Z, EDGE_POINTS + 2)
    rear_margin = rear_part(eigen_modes, 0, ELEMENTS_X)
    eigen_modes = jnp.einsum('epfbhg,pa->eafbhg', front_margin, basis[:EDGE_POINTS], precision=highest) + jnp.einsum('epfbhg,pa->eafbhg', rear_margin, basis[EDGE_POINTS:], precision=highest)
    lam_sum = eigen_values[:, None, None] + eigen_values[None, :, None] + eigen_values[None, None, :]
    divisor = viscous[:, None, :, None, :, None] * lam_sum[None, :, None, :, None, :] + reaction[:, None, :, None, :, None]
    eigen_modes = eigen_modes / divisor
    back_basis = basis[1:EDGE_POINTS + 1]
    local = jnp.einsum('eafbhg,qa->eqfbhg', eigen_modes, back_basis, precision=highest)
    local = jnp.einsum('eqfbhg,rb->eqfrhg', local, back_basis, precision=highest)
    local = jnp.einsum('eqfrhg,sg->eqfrhs', local, back_basis, precision=highest)
    return local.reshape(NX, NY, NZ)

def operate(field, viscous_pt, reaction_pt):
    padded_field = jnp.pad(field, 1)
    beside = padded_field[2:, 1:-1, 1:-1] + padded_field[:-2, 1:-1, 1:-1]
    beside = beside + padded_field[1:-1, 2:, 1:-1] + padded_field[1:-1, :-2, 1:-1]
    beside = beside + padded_field[1:-1, 1:-1, 2:] + padded_field[1:-1, 1:-1, :-2]
    return reaction_pt * field + viscous_pt * (6.0 * field - beside)

def reference(rhs, viscous, reaction):

    def single(field):
        first = precondition(field, viscous, reaction)
        residual = field - operate(first, expand(viscous), expand(reaction))
        return first + precondition(residual, viscous, reaction)
    return lax.map(single, rhs)
```

```python
import functools

import jax
import jax.numpy as jnp
import numpy as np
from jax import lax
from jax.experimental import pallas as pl
from jax.experimental.pallas import tpu as pltpu
from jax.sharding import PartitionSpec as P

EDGE = 16
SPAN = EDGE + 2
MODES = 384
ROWS = 160
MESH = pl.DeviceIdType.MESH
NT = (((1,), (1,)), ((), ()))
NN = (((1,), (0,)), ((), ()))
DIRS = [
    (dx, dy, dz)
    for dz in (0, -1, 1)
    for dy in (0, -1, 1)
    for dx in (0, -1, 1)
    if (dx, dy, dz) != (0, 0, 0)
]
Y_FIRST, Y_MID, Y_LAST, X_FIRST, X_LAST = 0, 16, 48, 64, 96


def tables():
    i = np.arange(SPAN)
    basis = np.sqrt(2.0 / (SPAN + 1)) * np.sin(np.pi * np.outer(i + 1, i + 1) / (SPAN + 1))
    lam = 2.0 - 2.0 * np.cos(np.pi * (i + 1) / (SPAN + 1))
    nz = 8
    z_fwd = np.zeros((ROWS, 128))
    z_back = np.zeros((nz * SPAN, 128))
    for h in range(nz):
        for z in range(128):
            w = z - EDGE * h + 1
            if 0 <= w < SPAN:
                z_fwd[h * SPAN : (h + 1) * SPAN, z] = basis[w]
            if 1 <= w <= EDGE:
                z_back[h * SPAN : (h + 1) * SPAN, z] = basis[w]
    z_fwd[nz * SPAN, 0] = 1.0
    z_fwd[nz * SPAN + 1, 127] = 1.0
    pair = np.zeros((SPAN, SPAN, MODES))
    for a in range(SPAN):
        for b in range(SPAN):
            pair[a, b, : SPAN * SPAN] = np.outer(basis[a], basis[b]).reshape(-1)
    main = pair[1:17, 1:17].reshape(256, MODES)
    shell = np.zeros((2, 128, MODES))
    for x in range(16):
        shell[0, Y_LAST + x] = pair[x + 1, 0]
        shell[0, 32 + x] = pair[x + 1, 17]
        shell[1, Y_FIRST + x] = pair[x + 1, 17]
        shell[1, Y_MID + x] = pair[x + 1, 0]
    for y in range(17):
        shell[0, X_FIRST + y] = pair[17, y + 1]
        shell[0, X_LAST + y] = pair[0, y + 1]
        shell[1, X_FIRST + 31 - y] = pair[17, 16 - y]
        shell[1, X_LAST + 31 - y] = pair[0, 16 - y]
    shell[0, X_FIRST + 31], shell[0, X_LAST + 31] = pair[17, 0], pair[0, 0]
    shell[1, X_FIRST], shell[1, X_LAST] = pair[17, 17], pair[0, 17]
    q = np.arange(nz * SPAN)
    first = np.where(q < SPAN, basis[0][q % SPAN], 0.0)
    last = np.where(q >= (nz - 1) * SPAN, basis[17][q % SPAN], 0.0)
    lam_z = lam[q % SPAN]
    columns = np.stack([np.repeat(v[:, None], 128, 1) for v in (first, last, lam_z)])
    lam_xy = np.zeros((8, MODES))
    lam_xy[:, : SPAN * SPAN] = (lam[:, None] + lam[None, :]).reshape(-1)
    f32 = functools.partial(np.asarray, dtype=np.float32)
    return f32(z_fwd), f32(z_back), f32(main), f32(shell), f32(columns), f32(lam_xy)


def halves(x):
    hi = x.astype(jnp.bfloat16)
    return hi, (x - hi.astype(jnp.float32)).astype(jnp.bfloat16)


def table_halves(x):
    hi = x.astype(jnp.bfloat16)
    return hi, (x - hi.astype(np.float32)).astype(jnp.bfloat16)


def constants():
    z_fwd, z_back, main, shell, columns, lam_xy = tables()
    zh, zl = table_halves(z_fwd)
    bh, bl = table_halves(z_back)
    mh, ml = table_halves(main)
    sh, sl = table_halves(shell)
    return (
        np.concatenate([zh, zh, zl], axis=1),
        np.stack([bh, bl]),
        np.concatenate([mh, mh, ml], axis=0),
        np.concatenate([sh, sh, sl], axis=1),
        np.concatenate([mh, mh, ml], axis=1),
        columns,
        lam_xy,
    )


def dot(a, b, dims):
    return lax.dot_general(a, b, dims, preferred_element_type=jnp.float32)


def kernel(
    sizes, rhs_hbm, visc_ref, reac_ref, zf_hbm, zb_hbm, km_hbm, ks_hbm, kb_hbm, col_hbm, lam_hbm,
    out_ref,
    rhs, first, resid, face, face_f, corner, zface, zedge,
    rx, ry, rc, rz, re, shell, z1h, z1l, inv,
    zf, zb, km, ks, kb, col, lam, load_sem, send_sem, recv_sem,
):
    axes = ("gx", "gy", "gz")
    me = tuple(lax.axis_index(a) for a in axes)

    def exists(d):
        ok = None
        for p, n, s in zip(me, sizes, d):
            if s:
                c = (p + s >= 0) & (p + s < n)
                ok = c if ok is None else ok & c
        return ok

    def peer(d):
        return tuple(p + s for p, s in zip(me, d))

    def minus(d):
        return tuple(-s for s in d)

    barrier = pltpu.get_barrier_semaphore()
    count = jnp.int32(0)
    for d in DIRS:
        ok = exists(d)
        count = count + ok.astype(jnp.int32)

        @pl.when(ok)
        def _(d=d):
            pl.semaphore_signal(barrier, inc=1, device_id=peer(d), device_id_type=MESH)

    loads = []
    for k, (src, dst) in enumerate(
        [(rhs_hbm, rhs), (zf_hbm, zf), (km_hbm, km), (ks_hbm, ks), (col_hbm, col), (lam_hbm, lam),
         (kb_hbm, kb), (zb_hbm, zb)]
    ):
        loads.append(pltpu.make_async_copy(src, dst, load_sem.at[k]))
        loads[-1].start()

    def pieces(rnd, d, face_ref):
        dx, dy, dz = d
        full = 0 if rnd == 0 else 1
        out = []
        if dz == 0 and dy == 0:
            lo = X_LAST if dx > 0 else X_FIRST
            out.append((face_ref.at[:, pl.ds(lo, 32), :], rx.at[rnd, int(dx > 0)]))
        elif dz == 0 and dx == 0:
            lo = Y_LAST if dy > 0 else Y_FIRST
            out.append((face_ref.at[:, pl.ds(lo, 16), :], ry.at[rnd, int(dy > 0)]))
        elif dz == 0:
            k = 2 * int(dx > 0) + int(dy > 0)
            out.append((corner.at[full, k], rc.at[full, k]))
        else:
            s = int(dz > 0)
            if dx == 0 and dy == 0:
                out.append((zface.at[rnd, s], rz.at[rnd, s]))
            if rnd != 1:
                out.append((zedge.at[full, s], re.at[full, s, 3 * (dx + 1) + dy + 1]))
        return out

    zface[...] = jnp.zeros(zface.shape, jnp.float32)
    started = {0: [], 1: [], 2: []}
    counter = [0]

    def send(rnd, dirs, face_ref):
        for d in dirs:
            copies = []
            for src, dst in pieces(rnd, d, face_ref):
                k = counter[0]
                counter[0] += 1
                copies.append(
                    pltpu.make_async_remote_copy(
                        src_ref=src, dst_ref=dst, send_sem=send_sem.at[k], recv_sem=recv_sem.at[k],
                        device_id=peer(d), device_id_type=MESH,
                    )
                )
                @pl.when(jnp.logical_not(exists(minus(d))))
                def _(dst=dst):
                    dst[...] = jnp.zeros(dst.shape, jnp.float32)

            @pl.when(exists(d))
            def _(copies=copies):
                for c in copies:
                    c.start()

            started[rnd].append((d, copies))

    def arrive(rnd):
        for d, copies in started[rnd]:
            @pl.when(exists(minus(d)))
            def _(copies=copies):
                for c in copies:
                    c.wait_recv()

    def drain(rnd):
        for d, copies in started[rnd]:
            @pl.when(exists(d))
            def _(copies=copies):
                for c in copies:
                    c.wait_send()

    def fill_face(src, dst):
        for c in range(3):
            for k, y in enumerate((0, 15, 16, 31)):
                dst[c, 16 * k : 16 * k + 16, :] = src[c, pl.ds(y, 16, stride=32), :]
            dst[c, X_FIRST : X_FIRST + 32, :] = src[c, 0:32]
            dst[c, X_LAST : X_LAST + 32, :] = src[c, 480:512]

    def fill_corner(full, face_ref):
        for k, row in enumerate((X_FIRST, X_FIRST + 31, X_LAST, X_LAST + 31)):
            for c in range(3):
                corner[full, k, c] = face_ref[c, row : row + 1, :]

    def z_forward(x):
        hi, lo = halves(x)
        two = jnp.concatenate([hi, lo], axis=1)
        return dot(zf[:, :256], two, NT) + dot(zf[:, 256:], hi, NT)

    def z_ends(x):
        hi, lo = halves(x)
        two = jnp.concatenate([hi, lo], axis=1)
        return dot(zf[144:, :256], two, NT)

    def store_halves(c, f, rows, lanes, x):
        hi, lo = halves(x)
        z1h[2 * c + f, rows, lanes] = hi
        z1l[2 * c + f, rows, lanes] = lo

    def main_part(src, rnd):
        def step(c, _):
            block = src[c].reshape(16, 32, 128)
            for f in range(2):
                m = z_forward(block[:, 16 * f : 16 * f + 16].reshape(256, 128))
                store_halves(c, f, slice(0, 144), slice(0, 256), m[:144])
                for s in range(2):
                    zface[rnd, s, pl.ds(2 * c + f, 1), :] = m[144 + s : 145 + s]
            return 0

        lax.fori_loop(0, 3, step, 0)

    def edges(full, face_ref):
        e = z_ends(face_ref[...].reshape(384, 128))
        for s in range(2):
            for c in range(3):
                zedge[full, s, c] = e[s : s + 1, 128 * c : 128 * c + 128]

    lane = lax.broadcasted_iota(jnp.int32, (1, 128), 1)

    def shells(full, rnd, face_ref):
        for c in range(3):
            for f in range(2):
                s = shell.at[c, f]
                s[0:16] = ry[rnd, 0, c]
                s[16:48] = face_ref[c, 16:48]
                s[48:64] = ry[rnd, 1, c]
                s[64:96] = rx[rnd, 0, c]
                s[96:128] = rx[rnd, 1, c]
                if f == 0:
                    s[95:96] = rc[full, 1, c]
                    s[127:128] = rc[full, 3, c]
                else:
                    s[64:65] = rc[full, 0, c]
                    s[96:97] = rc[full, 2, c]

    def slot(d):
        return 3 * (d[0] + 1) + d[1] + 1

    def shell_part(full, rnd):
        def step(c, _):
            m = z_forward(shell[c].reshape(256, 128))
            for f in range(2):
                store_halves(c, f, slice(0, 144), slice(256, 384), m[:144, 128 * f : 128 * f + 128])
            for f in range(2):
                main, ring = [], []
                for s in (1, 0):
                    main.append(rz[rnd, s, pl.ds(2 * c + f, 1), :])
                    got = lambda dx, dy: re[full, s, slot((dx, dy)), c]
                    t = got(0, 0)
                    if f == 0:
                        t = jnp.where((lane >= 48) & (lane < 64), got(0, 1), t)
                        t = jnp.where((lane >= 64) & (lane < 95), got(-1, 0), t)
                        t = jnp.where(lane == 95, got(-1, 1), t)
                        t = jnp.where((lane >= 96) & (lane < 127), got(1, 0), t)
                        t = jnp.where(lane == 127, got(1, 1), t)
                    else:
                        t = jnp.where(lane < 16, got(0, -1), t)
                        t = jnp.where(lane == 64, got(-1, -1), t)
                        t = jnp.where((lane > 64) & (lane < 96), got(-1, 0), t)
                        t = jnp.where(lane == 96, got(1, -1), t)
                        t = jnp.where(lane > 96, got(1, 0), t)
                    ring.append(t)
                pad = jnp.zeros((14, 384), jnp.float32)
                planes = jnp.concatenate(
                    [jnp.concatenate(main, axis=0), jnp.concatenate(ring, axis=0)], axis=1
                )
                planes = jnp.concatenate([planes, pad], axis=0)
                store_halves(c, f, slice(144, 160), slice(0, 384), planes)
            return 0

        lax.fori_loop(0, 3, step, 0)

    def joined(parts):
        return jnp.concatenate([p.reshape(16, 16, 128) for p in parts], axis=1).reshape(512, 128)

    def solve(put):
        def step(c, _):
            parts = []
            for f in range(2):
                k = 2 * c + f
                hi, lo = z1h[k], z1l[k]
                lhs = jnp.concatenate([hi[:, :256], lo[:, :256], hi[:, :256]], axis=1)
                ring = jnp.concatenate([hi[:, 256:], lo[:, 256:], hi[:, 256:]], axis=1)
                m = dot(lhs, km[...], NN) + dot(ring, ks[f], NN)
                wide = lambda v: jnp.concatenate([v] * 3, axis=1)
                t = m[:144] + wide(col[0]) * m[144:145] + wide(col[1]) * m[145:146]
                t = t * inv[f]
                hi, lo = halves(t)
                data = jnp.concatenate([hi, lo, hi], axis=1)
                u = dot(kb3(), data, NT)
                hi, lo = halves(u)
                parts.append(dot(hi, zb[0], NN) + dot(lo, zb[0], NN) + dot(hi, zb[1], NN))
            put(c, parts)
            return 0

        lax.fori_loop(0, 3, step, 0)

    def kb3():
        return kb[...]

    faces = [d for d in DIRS if sum(map(abs, d)) == 1]
    flat_dirs = [d for d in DIRS if d[2] == 0]
    z_dirs = [d for d in DIRS if d[2] != 0]

    loads[0].wait()
    fill_face(rhs, face.at[0])
    fill_corner(0, face.at[0])
    pl.semaphore_wait(barrier, count)
    send(0, flat_dirs, face.at[0])
    loads[1].wait()
    main_part(rhs, 0)
    edges(0, face.at[0])
    send(0, z_dirs, face.at[0])
    for k in range(2, 8):
        loads[k].wait()

    rows = lax.broadcasted_iota(jnp.int32, (144, 128), 0)
    for f in range(2):
        v = jnp.zeros((144, 128), jnp.float32)
        r = jnp.zeros((144, 128), jnp.float32)
        for h in range(8):
            at = (rows >= SPAN * h) & (rows < SPAN * h + SPAN)
            v = jnp.where(at, visc_ref[f, h], v)
            r = jnp.where(at, reac_ref[f, h], r)
        for t in range(3):
            part = slice(128 * t, 128 * t + 128)
            inv[f, :, part] = 1.0 / (v * (col[2] + lam[0:1, part]) + r)

    arrive(0)
    shells(0, 0, face.at[0])
    shell_part(0, 0)

    def put_first(c, parts):
        first[c] = joined(parts)

    solve(put_first)

    fill_face(first, face_f)
    flat_faces = [d for d in faces if d[2] == 0]
    send(1, flat_faces, face_f)

    def first_ends(c, _):
        block = first[c].reshape(16, 32, 128)
        for f in range(2):
            e = z_ends(block[:, 16 * f : 16 * f + 16].reshape(256, 128))
            for s in range(2):
                zface[1, s, pl.ds(2 * c + f, 1), :] = e[s : s + 1]
        return 0

    lax.fori_loop(0, 3, first_ends, 0)
    send(1, [d for d in faces if d[2] != 0], face_f)

    visc_z, reac_z = [], []
    for f in range(2):
        v = jnp.zeros((1, 128), jnp.float32)
        r = jnp.zeros((1, 128), jnp.float32)
        for h in range(8):
            at = (lane >= EDGE * h) & (lane < EDGE * h + EDGE)
            v = jnp.where(at, visc_ref[f, h], v)
            r = jnp.where(at, reac_ref[f, h], r)
        visc_z.append(v)
        reac_z.append(r)

    arrive(1)
    drain(0)

    y_index = lax.broadcasted_iota(jnp.int32, (16, 32, 128), 1)
    z_index = lax.broadcasted_iota(jnp.int32, (16, 32, 128), 2)
    visc_b = jnp.where(y_index < 16, visc_z[0].reshape(1, 1, 128), visc_z[1].reshape(1, 1, 128))
    reac_b = jnp.where(y_index < 16, reac_z[0].reshape(1, 1, 128), reac_z[1].reshape(1, 1, 128))
    below = jnp.transpose(jnp.concatenate([rz[1, 1], rz[1, 0]], axis=0))
    for c in range(3):
        x = first[c].reshape(16, 32, 128)
        beside = jnp.concatenate([rx[1, 1, c][None], x[:15]], axis=0)
        beside = beside + jnp.concatenate([x[1:], rx[1, 0, c][None]], axis=0)
        ylo, yhi = (jnp.broadcast_to(ry[1, s, c][:, None, :], (16, 32, 128)) for s in (1, 0))
        beside = beside + jnp.where(y_index == 0, ylo, pltpu.roll(x, 1, 1))
        beside = beside + jnp.where(y_index == 31, yhi, pltpu.roll(x, 31, 1))
        zlo, zhi = (
            jnp.concatenate(
                [
                    jnp.broadcast_to(below[:, k : k + 1], (256, 128)).reshape(16, 16, 128)
                    for k in (8 * s + 2 * c, 8 * s + 2 * c + 1)
                ],
                axis=1,
            )
            for s in (0, 1)
        )
        beside = beside + jnp.where(z_index == 0, zlo, pltpu.roll(x, 1, 2))
        beside = beside + jnp.where(z_index == 127, zhi, pltpu.roll(x, 127, 2))
        applied = reac_b * x + visc_b * (6.0 * x - beside)
        resid[c] = rhs[c] - applied.reshape(512, 128)

    fill_face(resid, face.at[1])
    fill_corner(1, face.at[1])
    send(2, flat_dirs, face.at[1])
    main_part(resid, 2)
    edges(1, face.at[1])
    send(2, z_dirs, face.at[1])
    drain(1)
    arrive(2)
    shells(1, 2, face.at[1])
    shell_part(1, 2)

    def put_last(c, parts):
        out_ref[c] = first[c] + joined(parts)

    solve(put_last)
    drain(2)


def shards(sizes, rhs, viscous, reaction):
    f32, bf16 = jnp.float32, jnp.bfloat16
    consts = constants()
    any_space = pl.BlockSpec(memory_space=pl.ANY)
    smem = pl.BlockSpec(memory_space=pltpu.SMEM)
    vmem = pl.BlockSpec(memory_space=pltpu.VMEM)
    copies = 28 * 2 + 6
    scratch = [
        pltpu.VMEM((3, 512, 128), f32),
        pltpu.VMEM((3, 512, 128), f32),
        pltpu.VMEM((3, 512, 128), f32),
        pltpu.VMEM((2, 3, 128, 128), f32),
        pltpu.VMEM((3, 128, 128), f32),
        pltpu.VMEM((2, 4, 3, 1, 128), f32),
        pltpu.VMEM((3, 2, 8, 256), f32),
        pltpu.VMEM((2, 2, 3, 1, 128), f32),
        pltpu.VMEM((3, 2, 3, 32, 128), f32),
        pltpu.VMEM((3, 2, 3, 16, 128), f32),
        pltpu.VMEM((2, 4, 3, 1, 128), f32),
        pltpu.VMEM((3, 2, 8, 256), f32),
        pltpu.VMEM((2, 2, 9, 3, 1, 128), f32),
        pltpu.VMEM((3, 2, 128, 128), f32),
        pltpu.VMEM((6, ROWS, MODES), bf16),
        pltpu.VMEM((6, ROWS, MODES), bf16),
        pltpu.VMEM((2, 144, MODES), f32),
    ]
    scratch += [pltpu.VMEM(t.shape, t.dtype) for t in consts]
    scratch += [
        pltpu.SemaphoreType.DMA((8,)),
        pltpu.SemaphoreType.DMA((copies,)),
        pltpu.SemaphoreType.DMA((copies,)),
    ]
    out = pl.pallas_call(
        functools.partial(kernel, sizes),
        out_shape=jax.ShapeDtypeStruct((3, 512, 128), f32),
        in_specs=[any_space, smem, smem] + [any_space] * len(consts),
        out_specs=vmem,
        scratch_shapes=scratch,
        compiler_params=pltpu.CompilerParams(
            collective_id=0, has_side_effects=True, vmem_limit_bytes=48 * 2**20
        ),
    )(rhs.reshape(3, 512, 128), viscous.reshape(2, 8), reaction.reshape(2, 8), *consts)
    return out.reshape(rhs.shape)


def solution(mesh):
    sizes = tuple(mesh.shape[a] for a in ("gx", "gy", "gz"))
    placed = (P(None, "gx", "gy", "gz"), P("gx", "gy", "gz"), P("gx", "gy", "gz"))
    return jax.shard_map(
        functools.partial(shards, sizes),
        mesh=mesh,
        in_specs=placed,
        out_specs=P(None, "gx", "gy", "gz"),
        check_vma=False,
    )
```

```python
import functools

import jax
import jax.numpy as jnp
import numpy as np
from jax import lax
from jax.experimental import pallas as pl
from jax.experimental.pallas import tpu as pltpu
from jax.sharding import PartitionSpec as P

EDGE = 16
SPAN = EDGE + 2
MODES = 384
ROWS = 160
MESH = pl.DeviceIdType.MESH
NT = (((1,), (1,)), ((), ()))
NN = (((1,), (0,)), ((), ()))
DIRS = [
    (dx, dy, dz)
    for dz in (0, -1, 1)
    for dy in (0, -1, 1)
    for dx in (0, -1, 1)
    if (dx, dy, dz) != (0, 0, 0)
]
Y_FIRST, Y_MID, Y_LAST, X_FIRST, X_LAST = 0, 16, 48, 64, 96


def tables():
    i = np.arange(SPAN)
    basis = np.sqrt(2.0 / (SPAN + 1)) * np.sin(np.pi * np.outer(i + 1, i + 1) / (SPAN + 1))
    lam = 2.0 - 2.0 * np.cos(np.pi * (i + 1) / (SPAN + 1))
    nz = 8
    z_fwd = np.zeros((ROWS, 128))
    z_back = np.zeros((nz * SPAN, 128))
    for h in range(nz):
        for z in range(128):
            w = z - EDGE * h + 1
            if 0 <= w < SPAN:
                z_fwd[h * SPAN : (h + 1) * SPAN, z] = basis[w]
            if 1 <= w <= EDGE:
                z_back[h * SPAN : (h + 1) * SPAN, z] = basis[w]
    z_fwd[nz * SPAN, 0] = 1.0
    z_fwd[nz * SPAN + 1, 127] = 1.0
    pair = np.zeros((SPAN, SPAN, MODES))
    for a in range(SPAN):
        for b in range(SPAN):
            pair[a, b, : SPAN * SPAN] = np.outer(basis[a], basis[b]).reshape(-1)
    main = pair[1:17, 1:17].reshape(256, MODES)
    shell = np.zeros((2, 128, MODES))
    for x in range(16):
        shell[0, Y_LAST + x] = pair[x + 1, 0]
        shell[0, 32 + x] = pair[x + 1, 17]
        shell[1, Y_FIRST + x] = pair[x + 1, 17]
        shell[1, Y_MID + x] = pair[x + 1, 0]
    for y in range(17):
        shell[0, X_FIRST + y] = pair[17, y + 1]
        shell[0, X_LAST + y] = pair[0, y + 1]
        shell[1, X_FIRST + 31 - y] = pair[17, 16 - y]
        shell[1, X_LAST + 31 - y] = pair[0, 16 - y]
    shell[0, X_FIRST + 31], shell[0, X_LAST + 31] = pair[17, 0], pair[0, 0]
    shell[1, X_FIRST], shell[1, X_LAST] = pair[17, 17], pair[0, 17]
    q = np.arange(nz * SPAN)
    first = np.where(q < SPAN, basis[0][q % SPAN], 0.0)
    last = np.where(q >= (nz - 1) * SPAN, basis[17][q % SPAN], 0.0)
    lam_z = lam[q % SPAN]
    columns = np.stack([np.repeat(v[:, None], 128, 1) for v in (first, last, lam_z)])
    lam_xy = np.zeros((8, MODES))
    lam_xy[:, : SPAN * SPAN] = (lam[:, None] + lam[None, :]).reshape(-1)
    f32 = functools.partial(np.asarray, dtype=np.float32)
    return f32(z_fwd), f32(z_back), f32(main), f32(shell), f32(columns), f32(lam_xy)


def halves(x):
    hi = x.astype(jnp.bfloat16)
    return hi, (x - hi.astype(jnp.float32)).astype(jnp.bfloat16)


def table_halves(x):
    hi = x.astype(jnp.bfloat16)
    return hi, (x - hi.astype(np.float32)).astype(jnp.bfloat16)


def constants():
    z_fwd, z_back, main, shell, columns, lam_xy = tables()
    zh, zl = table_halves(z_fwd)
    bh, bl = table_halves(z_back)
    mh, ml = table_halves(main)
    sh, sl = table_halves(shell)
    return (
        np.concatenate([zh, zh, zl], axis=1),
        np.stack([bh, bl]),
        np.concatenate([mh, mh, ml], axis=0),
        np.concatenate([sh, sh, sl], axis=1),
        np.concatenate([mh, mh, ml], axis=1),
        columns,
        lam_xy,
    )


def dot(a, b, dims):
    return lax.dot_general(a, b, dims, preferred_element_type=jnp.float32)


def kernel(
    sizes, rhs_hbm, visc_ref, reac_ref, zf_hbm, zb_hbm, km_hbm, ks_hbm, kb_hbm, col_hbm, lam_hbm,
    out_ref,
    rhs, first, resid, face, face_f, corner, zface, zedge,
    rx, ry, rc, rz, re, shell, z1h, z1l, inv,
    zf, zb, km, ks, kb, col, lam, load_sem, send_sem, recv_sem,
):
    axes = ("gx", "gy", "gz")
    me = tuple(lax.axis_index(a) for a in axes)

    def exists(d):
        ok = None
        for p, n, s in zip(me, sizes, d):
            if s:
                c = (p + s >= 0) & (p + s < n)
                ok = c if ok is None else ok & c
        return ok

    def peer(d):
        return tuple(p + s for p, s in zip(me, d))

    def minus(d):
        return tuple(-s for s in d)

    barrier = pltpu.get_barrier_semaphore()
    count = jnp.int32(0)
    for d in DIRS:
        ok = exists(d)
        count = count + ok.astype(jnp.int32)

        @pl.when(ok)
        def _(d=d):
            pl.semaphore_signal(barrier, inc=1, device_id=peer(d), device_id_type=MESH)

    loads = []
    for k, (src, dst) in enumerate(
        [(rhs_hbm, rhs), (zf_hbm, zf), (km_hbm, km), (ks_hbm, ks), (col_hbm, col), (lam_hbm, lam),
         (kb_hbm, kb), (zb_hbm, zb)]
    ):
        loads.append(pltpu.make_async_copy(src, dst, load_sem.at[k]))
        loads[-1].start()

    def pieces(rnd, d, face_ref):
        dx, dy, dz = d
        full = 0 if rnd == 0 else 1
        out = []
        if dz == 0 and dy == 0:
            lo = X_LAST if dx > 0 else X_FIRST
            out.append((face_ref.at[:, pl.ds(lo, 32), :], rx.at[rnd, int(dx > 0)]))
        elif dz == 0 and dx == 0:
            lo = Y_LAST if dy > 0 else Y_FIRST
            out.append((face_ref.at[:, pl.ds(lo, 16), :], ry.at[rnd, int(dy > 0)]))
        elif dz == 0:
            k = 2 * int(dx > 0) + int(dy > 0)
            out.append((corner.at[full, k], rc.at[full, k]))
        else:
            s = int(dz > 0)
            if dx == 0 and dy == 0:
                out.append((zface.at[rnd, s], rz.at[rnd, s]))
            if rnd != 1:
                out.append((zedge.at[full, s], re.at[full, s, 3 * (dx + 1) + dy + 1]))
        return out

    zface[...] = jnp.zeros(zface.shape, jnp.float32)
    started = {0: [], 1: [], 2: []}
    counter = [0]

    def send(rnd, dirs, face_ref):
        for d in dirs:
            copies = []
            for src, dst in pieces(rnd, d, face_ref):
                k = counter[0]
                counter[0] += 1
                copies.append(
                    pltpu.make_async_remote_copy(
                        src_ref=src, dst_ref=dst, send_sem=send_sem.at[k], recv_sem=recv_sem.at[k],
                        device_id=peer(d), device_id_type=MESH,
                    )
                )
                @pl.when(jnp.logical_not(exists(minus(d))))
                def _(dst=dst):
                    dst[...] = jnp.zeros(dst.shape, jnp.float32)

            @pl.when(exists(d))
            def _(copies=copies):
                for c in copies:
                    c.start()

            started[rnd].append((d, copies))

    def arrive(rnd):
        for d, copies in started[rnd]:
            @pl.when(exists(minus(d)))
            def _(copies=copies):
                for c in copies:
                    c.wait_recv()

    def drain(rnd):
        for d, copies in started[rnd]:
            @pl.when(exists(d))
            def _(copies=copies):
                for c in copies:
                    c.wait_send()

    def fill_face(src, dst):
        for c in range(3):
            for k, y in enumerate((0, 15, 16, 31)):
                dst[c, 16 * k : 16 * k + 16, :] = src[c, pl.ds(y, 16, stride=32), :]
            dst[c, X_FIRST : X_FIRST + 32, :] = src[c, 0:32]
            dst[c, X_LAST : X_LAST + 32, :] = src[c, 480:512]

    def fill_corner(full, face_ref):
        for k, row in enumerate((X_FIRST, X_FIRST + 31, X_LAST, X_LAST + 31)):
            for c in range(3):
                corner[full, k, c] = face_ref[c, row : row + 1, :]

    def z_forward(x):
        hi, lo = halves(x)
        two = jnp.concatenate([hi, lo], axis=1)
        return dot(zf[:, :256], two, NT) + dot(zf[:, 256:], hi, NT)

    def z_ends(x):
        hi, lo = halves(x)
        two = jnp.concatenate([hi, lo], axis=1)
        return dot(zf[144:, :256], two, NT)

    def store_halves(c, f, rows, lanes, x):
        hi, lo = halves(x)
        z1h[2 * c + f, rows, lanes] = hi
        z1l[2 * c + f, rows, lanes] = lo

    def main_part(src, rnd):
        def step(c, _):
            block = src[c].reshape(16, 32, 128)
            for f in range(2):
                m = z_forward(block[:, 16 * f : 16 * f + 16].reshape(256, 128))
                store_halves(c, f, slice(0, 144), slice(0, 256), m[:144])
                for s in range(2):
                    zface[rnd, s, pl.ds(2 * c + f, 1), :] = m[144 + s : 145 + s]
            return 0

        lax.fori_loop(0, 3, step, 0)

    def edges(full, face_ref):
        e = z_ends(face_ref[...].reshape(384, 128))
        for s in range(2):
            for c in range(3):
                zedge[full, s, c] = e[s : s + 1, 128 * c : 128 * c + 128]

    lane = lax.broadcasted_iota(jnp.int32, (1, 128), 1)

    def shells(full, rnd, face_ref):
        for c in range(3):
            for f in range(2):
                s = shell.at[c, f]
                s[0:16] = ry[rnd, 0, c]
                s[16:48] = face_ref[c, 16:48]
                s[48:64] = ry[rnd, 1, c]
                s[64:96] = rx[rnd, 0, c]
                s[96:128] = rx[rnd, 1, c]
                if f == 0:
                    s[95:96] = rc[full, 1, c]
                    s[127:128] = rc[full, 3, c]
                else:
                    s[64:65] = rc[full, 0, c]
                    s[96:97] = rc[full, 2, c]

    def slot(d):
        return 3 * (d[0] + 1) + d[1] + 1

    def shell_part(full, rnd):
        def step(c, _):
            m = z_forward(shell[c].reshape(256, 128))
            for f in range(2):
                store_halves(c, f, slice(0, 144), slice(256, 384), m[:144, 128 * f : 128 * f + 128])
            for f in range(2):
                main, ring = [], []
                for s in (1, 0):
                    main.append(rz[rnd, s, pl.ds(2 * c + f, 1), :])
                    got = lambda dx, dy: re[full, s, slot((dx, dy)), c]
                    t = got(0, 0)
                    if f == 0:
                        t = jnp.where((lane >= 48) & (lane < 64), got(0, 1), t)
                        t = jnp.where((lane >= 64) & (lane < 95), got(-1, 0), t)
                        t = jnp.where(lane == 95, got(-1, 1), t)
                        t = jnp.where((lane >= 96) & (lane < 127), got(1, 0), t)
                        t = jnp.where(lane == 127, got(1, 1), t)
                    else:
                        t = jnp.where(lane < 16, got(0, -1), t)
                        t = jnp.where(lane == 64, got(-1, -1), t)
                        t = jnp.where((lane > 64) & (lane < 96), got(-1, 0), t)
                        t = jnp.where(lane == 96, got(1, -1), t)
                        t = jnp.where(lane > 96, got(1, 0), t)
                    ring.append(t)
                pad = jnp.zeros((14, 384), jnp.float32)
                planes = jnp.concatenate(
                    [jnp.concatenate(main, axis=0), jnp.concatenate(ring, axis=0)], axis=1
                )
                planes = jnp.concatenate([planes, pad], axis=0)
                store_halves(c, f, slice(144, 160), slice(0, 384), planes)
            return 0

        lax.fori_loop(0, 3, step, 0)

    def joined(parts):
        return jnp.concatenate([p.reshape(16, 16, 128) for p in parts], axis=1).reshape(512, 128)

    def solve(put):
        def step(c, _):
            parts = []
            for f in range(2):
                k = 2 * c + f
                hi, lo = z1h[k], z1l[k]
                lhs = jnp.concatenate([hi[:, :256], lo[:, :256], hi[:, :256]], axis=1)
                ring = jnp.concatenate([hi[:, 256:], lo[:, 256:], hi[:, 256:]], axis=1)
                m = dot(lhs, km[...], NN) + dot(ring, ks[f], NN)
                wide = lambda v: jnp.concatenate([v] * 3, axis=1)
                t = m[:144] + wide(col[0]) * m[144:145] + wide(col[1]) * m[145:146]
                t = t * inv[f]
                hi, lo = halves(t)
                data = jnp.concatenate([hi, lo, hi], axis=1)
                u = dot(kb3(), data, NT)
                hi, lo = halves(u)
                parts.append(dot(hi, zb[0], NN) + dot(lo, zb[0], NN) + dot(hi, zb[1], NN))
            put(c, parts)
            return 0

        lax.fori_loop(0, 3, step, 0)

    def kb3():
        return kb[...]

    faces = [d for d in DIRS if sum(map(abs, d)) == 1]
    flat_dirs = [d for d in DIRS if d[2] == 0]
    z_dirs = [d for d in DIRS if d[2] != 0]

    loads[0].wait()
    fill_face(rhs, face.at[0])
    fill_corner(0, face.at[0])
    pl.semaphore_wait(barrier, count)
    send(0, flat_dirs, face.at[0])
    loads[1].wait()
    main_part(rhs, 0)
    edges(0, face.at[0])
    send(0, z_dirs, face.at[0])
    for k in range(2, 8):
        loads[k].wait()

    rows = lax.broadcasted_iota(jnp.int32, (144, 128), 0)
    for f in range(2):
        v = jnp.zeros((144, 128), jnp.float32)
        r = jnp.zeros((144, 128), jnp.float32)
        for h in range(8):
            at = (rows >= SPAN * h) & (rows < SPAN * h + SPAN)
            v = jnp.where(at, visc_ref[f, h], v)
            r = jnp.where(at, reac_ref[f, h], r)
        for t in range(3):
            part = slice(128 * t, 128 * t + 128)
            inv[f, :, part] = 1.0 / (v * (col[2] + lam[0:1, part]) + r)

    arrive(0)
    shells(0, 0, face.at[0])
    shell_part(0, 0)

    def put_first(c, parts):
        first[c] = joined(parts)

    solve(put_first)

    fill_face(first, face_f)
    flat_faces = [d for d in faces if d[2] == 0]
    send(1, flat_faces, face_f)

    def first_ends(c, _):
        block = first[c].reshape(16, 32, 128)
        for f in range(2):
            e = z_ends(block[:, 16 * f : 16 * f + 16].reshape(256, 128))
            for s in range(2):
                zface[1, s, pl.ds(2 * c + f, 1), :] = e[s : s + 1]
        return 0

    lax.fori_loop(0, 3, first_ends, 0)
    send(1, [d for d in faces if d[2] != 0], face_f)

    visc_z, reac_z = [], []
    for f in range(2):
        v = jnp.zeros((1, 128), jnp.float32)
        r = jnp.zeros((1, 128), jnp.float32)
        for h in range(8):
            at = (lane >= EDGE * h) & (lane < EDGE * h + EDGE)
            v = jnp.where(at, visc_ref[f, h], v)
            r = jnp.where(at, reac_ref[f, h], r)
        visc_z.append(v)
        reac_z.append(r)

    arrive(1)
    drain(0)

    y_index = lax.broadcasted_iota(jnp.int32, (16, 32, 128), 1)
    z_index = lax.broadcasted_iota(jnp.int32, (16, 32, 128), 2)
    visc_b = jnp.where(y_index < 16, visc_z[0].reshape(1, 1, 128), visc_z[1].reshape(1, 1, 128))
    reac_b = jnp.where(y_index < 16, reac_z[0].reshape(1, 1, 128), reac_z[1].reshape(1, 1, 128))
    below = jnp.transpose(jnp.concatenate([rz[1, 1], rz[1, 0]], axis=0))
    for c in range(3):
        x = first[c].reshape(16, 32, 128)
        beside = jnp.concatenate([rx[1, 1, c][None], x[:15]], axis=0)
        beside = beside + jnp.concatenate([x[1:], rx[1, 0, c][None]], axis=0)
        ylo, yhi = (jnp.broadcast_to(ry[1, s, c][:, None, :], (16, 32, 128)) for s in (1, 0))
        beside = beside + jnp.where(y_index == 0, ylo, pltpu.roll(x, 1, 1))
        beside = beside + jnp.where(y_index == 31, yhi, pltpu.roll(x, 31, 1))
        zlo, zhi = (
            jnp.concatenate(
                [
                    jnp.broadcast_to(below[:, k : k + 1], (256, 128)).reshape(16, 16, 128)
                    for k in (8 * s + 2 * c, 8 * s + 2 * c + 1)
                ],
                axis=1,
            )
            for s in (0, 1)
        )
        beside = beside + jnp.where(z_index == 0, zlo, pltpu.roll(x, 1, 2))
        beside = beside + jnp.where(z_index == 127, zhi, pltpu.roll(x, 127, 2))
        applied = reac_b * x + visc_b * (6.0 * x - beside)
        resid[c] = rhs[c] - applied.reshape(512, 128)

    fill_face(resid, face.at[1])
    fill_corner(1, face.at[1])
    send(2, flat_dirs, face.at[1])
    main_part(resid, 2)
    edges(1, face.at[1])
    send(2, z_dirs, face.at[1])
    drain(1)
    arrive(2)
    shells(1, 2, face.at[1])
    shell_part(1, 2)

    def put_last(c, parts):
        out_ref[c] = first[c] + joined(parts)

    solve(put_last)
    drain(2)


def shards(sizes, rhs, viscous, reaction):
    f32, bf16 = jnp.float32, jnp.bfloat16
    consts = constants()
    any_space = pl.BlockSpec(memory_space=pltpu.HBM)
    smem = pl.BlockSpec(memory_space=pltpu.SMEM)
    vmem = pl.BlockSpec(memory_space=pltpu.VMEM)
    copies = 28 * 2 + 6
    scratch = [
        pltpu.VMEM((3, 512, 128), f32),
        pltpu.VMEM((3, 512, 128), f32),
        pltpu.VMEM((3, 512, 128), f32),
        pltpu.VMEM((2, 3, 128, 128), f32),
        pltpu.VMEM((3, 128, 128), f32),
        pltpu.VMEM((2, 4, 3, 1, 128), f32),
        pltpu.VMEM((3, 2, 8, 256), f32),
        pltpu.VMEM((2, 2, 3, 1, 128), f32),
        pltpu.VMEM((3, 2, 3, 32, 128), f32),
        pltpu.VMEM((3, 2, 3, 16, 128), f32),
        pltpu.VMEM((2, 4, 3, 1, 128), f32),
        pltpu.VMEM((3, 2, 8, 256), f32),
        pltpu.VMEM((2, 2, 9, 3, 1, 128), f32),
        pltpu.VMEM((3, 2, 128, 128), f32),
        pltpu.VMEM((6, ROWS, MODES), bf16),
        pltpu.VMEM((6, ROWS, MODES), bf16),
        pltpu.VMEM((2, 144, MODES), f32),
    ]
    scratch += [pltpu.VMEM(t.shape, t.dtype) for t in consts]
    scratch += [
        pltpu.SemaphoreType.DMA((8,)),
        pltpu.SemaphoreType.DMA((copies,)),
        pltpu.SemaphoreType.DMA((copies,)),
    ]
    out = pl.pallas_call(
        functools.partial(kernel, sizes),
        out_shape=jax.ShapeDtypeStruct((3, 512, 128), f32),
        in_specs=[any_space, smem, smem] + [any_space] * len(consts),
        out_specs=vmem,
        scratch_shapes=scratch,
        compiler_params=pltpu.CompilerParams(
            collective_id=0, has_side_effects=True, vmem_limit_bytes=67043328
        ),
    )(rhs.reshape(3, 512, 128), viscous.reshape(2, 8), reaction.reshape(2, 8), *consts)
    return out.reshape(rhs.shape)


def solution(mesh):
    sizes = tuple(mesh.shape[a] for a in ("gx", "gy", "gz"))
    placed = (P(None, "gx", "gy", "gz"), P("gx", "gy", "gz"), P("gx", "gy", "gz"))
    return jax.shard_map(
        functools.partial(shards, sizes),
        mesh=mesh,
        in_specs=placed,
        out_specs=P(None, "gx", "gy", "gz"),
        check_vma=False,
    )
```

```python
import functools

import jax
import jax.numpy as jnp
import numpy as np
from jax import lax
from jax.experimental import pallas as pl
from jax.experimental.pallas import tpu as pltpu
from jax.sharding import PartitionSpec as P

EDGE = 16
SPAN = EDGE + 2
HALF = 168
RING = 40
LOW, HIGH = 56, 60
MESH = pl.DeviceIdType.MESH
NN = (((1,), (0,)), ((), ()))
DIRS = [
    (dx, dy, dz)
    for dz in (0, -1, 1)
    for dy in (0, -1, 1)
    for dx in (0, -1, 1)
    if (dx, dy, dz) != (0, 0, 0)
]
FACES = [d for d in DIRS if sum(map(abs, d)) == 1]
Y_FIRST, Y_MID, Y_LAST, X_FIRST, X_LAST = 0, 16, 48, 64, 96


def table_halves(x):
    x = x.astype(np.float32)
    hi = x.astype(jnp.bfloat16)
    return hi, (x - hi.astype(np.float32)).astype(jnp.bfloat16)


def constants():
    i = np.arange(SPAN)
    basis = np.sqrt(2.0 / (SPAN + 1)) * np.sin(np.pi * np.outer(i + 1, i + 1) / (SPAN + 1))
    lam = 2.0 - 2.0 * np.cos(np.pi * (i + 1) / (SPAN + 1))
    q = np.arange(144)
    lanes = np.concatenate([np.arange(128), np.tile(np.arange(128, 144), 3)])
    forward = np.zeros((128, 256))
    back = np.zeros((144, 128))
    for h in range(8):
        for z in range(128):
            w = z - EDGE * h + 1
            if 0 <= w < SPAN:
                for n, k in enumerate(lanes):
                    if k // SPAN == h:
                        forward[z, n] = basis[w, k % SPAN]
            if 1 <= w <= EDGE:
                back[h * SPAN : (h + 1) * SPAN, z] = basis[w]
    forward[0, 128 + LOW] = 1.0
    forward[127, 128 + HIGH] = 1.0
    wide = np.zeros((144, 256))
    wide[:, :128] = back
    wide[:, 128 + LOW] = 2.0 * back[:, 0]
    wide[:, 128 + HIGH] = 2.0 * back[:, 127]
    fh, fl = table_halves(forward)
    bh, bl = table_halves(wide)
    z_forward = np.concatenate([fh, fh, fl], axis=0)
    z_back = np.concatenate(
        [bh[:128], bh[:128], bl[:128], bh[128:], bh[128:], bl[128:], np.zeros((80, 256), bh.dtype)], axis=0
    )
    into, out_of, lam_xy = [], [], []
    for parity in range(2):
        mode = np.arange(162)
        a, b = 2 * (mode // SPAN) + parity, mode % SPAN
        point = lambda x, y: basis[x, a] * basis[y, b]
        main = np.zeros((176, 128))
        for x in range(8):
            for y in range(16):
                main[:162, 16 * x + y] = point(x + 1, y + 1)
        ring = np.zeros((176, RING))
        for y in range(16):
            ring[:162, y] = point(0, y + 1)
        for x in range(8):
            ring[:162, 16 + x] = point(x + 1, 0)
            ring[:162, 24 + x] = point(x + 1, 17)
        ring[:162, 32], ring[:162, 33] = point(0, 0), point(0, 17)
        mh, ml = table_halves(main)
        rh, rl = table_halves(ring)
        into.append(np.concatenate([mh, mh, ml, rh, rh, rl, np.zeros((176, 8), mh.dtype)], axis=1))
        th, tl = mh[:HALF].T, ml[:HALF].T
        out_of.append(np.concatenate([th, th, tl, np.zeros((128, 8), mh.dtype)], axis=1))
        col = np.zeros((HALF, 1))
        col[:162, 0] = lam[a] + lam[b]
        lam_xy.append(np.repeat(col, 128, 1))
    rows = np.zeros((8, 256))
    for n, k in enumerate(lanes):
        if k < SPAN:
            rows[0, n], rows[2, n] = basis[0, k], basis[1, k]
        if k >= 7 * SPAN:
            rows[1, n], rows[3, n] = basis[17, k % SPAN], basis[16, k % SPAN]
        rows[4, n] = lam[k % SPAN]
    f32 = functools.partial(np.asarray, dtype=np.float32)
    return z_forward, np.stack(into), np.stack(out_of), z_back, f32(rows), f32(np.stack(lam_xy))


def dot(a, b):
    return lax.dot_general(a, b, NN, preferred_element_type=jnp.float32)


def halves(x):
    hi = x.astype(jnp.bfloat16)
    return hi, (x - hi.astype(jnp.float32)).astype(jnp.bfloat16)


def wide_halves(x):
    hi = x.astype(jnp.bfloat16).astype(jnp.float32)
    return hi, x - hi


def kernel(
    sizes, rhs_hbm, visc_hbm, reac_hbm, zf_hbm, into_hbm, outof_hbm, zb_hbm, row_hbm, lam_hbm,
    out_ref,
    rhs, first, resid, face, corner, zsend, zedge, rx, ry, rc, rz, re,
    part_hi, part_lo, part_end, ring, ring_end, inv, visc_plane, coef_plane,
    zf, into, outof, zb, row, lam, visc_ref, reac_ref, load_sem, send_sem, recv_sem,
):
    me = tuple(lax.axis_index(a) for a in ("gx", "gy", "gz"))

    def exists(d):
        ok = None
        for p, n, s in zip(me, sizes, d):
            if s:
                c = (p + s >= 0) & (p + s < n)
                ok = c if ok is None else ok & c
        return ok

    def peer(d):
        return tuple(p + s for p, s in zip(me, d))

    def minus(d):
        return tuple(-s for s in d)

    barrier = pltpu.get_barrier_semaphore()
    count = jnp.int32(0)
    for d in DIRS:
        ok = exists(d)
        count = count + ok.astype(jnp.int32)

        @pl.when(ok)
        def _(d=d):
            pl.semaphore_signal(barrier, inc=1, device_id=peer(d), device_id_type=MESH)

    loads = []
    pairs = [(rhs_hbm.at[c], rhs.at[c]) for c in range(3)]
    pairs += [(zf_hbm, zf), (visc_hbm, visc_ref), (reac_hbm, reac_ref), (row_hbm, row), (lam_hbm, lam), (into_hbm, into), (outof_hbm, outof), (zb_hbm, zb)]
    for k, (src, dst) in enumerate(pairs):
        loads.append(pltpu.make_async_copy(src, dst, load_sem.at[k]))
        loads[-1].start()

    def pieces(rnd, c, d):
        dx, dy, dz = d
        full = 0 if rnd == 0 else 1
        if dz == 0 and dy == 0:
            return face.at[rnd, c, pl.ds(X_LAST if dx > 0 else X_FIRST, 32), :], rx.at[rnd, int(dx > 0), c]
        if dz == 0 and dx == 0:
            return face.at[rnd, c, pl.ds(Y_LAST if dy > 0 else Y_FIRST, 16), :], ry.at[rnd, int(dy > 0), c]
        if dz == 0:
            k = 2 * int(dx > 0) + int(dy > 0)
            return corner.at[full, k, c], rc.at[full, k, c]
        s = int(dz > 0)
        if dx == 0 and dy == 0:
            return zsend.at[rnd, s, c], rz.at[rnd, s, c]
        return zedge.at[full, s, c], re.at[full, s, slot(d), c]

    def slot(d):
        return 3 * (d[0] + 1) + d[1] + 1

    copies = {}
    for rnd in range(3):
        for c in range(3):
            for d in DIRS if rnd != 1 else FACES:
                k = len(copies)
                src, dst = pieces(rnd, c, d)
                copies[rnd, c, d] = pltpu.make_async_remote_copy(
                    src_ref=src, dst_ref=dst, send_sem=send_sem.at[k], recv_sem=recv_sem.at[k],
                    device_id=peer(d), device_id_type=MESH,
                )

    def send(rnd, c, ask):
        for (r, cc, d), copy in copies.items():
            if r == rnd and cc == c and ask(d):
                pl.when(exists(d))(copy.start)

    def arrive(rnd, c, ask=lambda d: True):
        for (r, cc, d), copy in copies.items():
            if r == rnd and cc == c and ask(d):
                pl.when(exists(minus(d)))(copy.wait_recv)

    flat = lambda d: d[2] == 0
    deep = lambda d: d[2] != 0

    for d in DIRS:
        @pl.when(jnp.logical_not(exists(minus(d))))
        def _(d=d):
            for rnd in range(3):
                if rnd != 1 or d in FACES:
                    for c in range(3):
                        dst = pieces(rnd, c, d)[1]
                        dst[...] = jnp.zeros(dst.shape, jnp.float32)

    zsend[...] = jnp.zeros(zsend.shape, jnp.float32)
    for k in range(4):
        ring[k, 32:40] = jnp.zeros((8, 128), jnp.float32)
        ring_end[k, 32:40] = jnp.zeros((8, 128), jnp.float32)

    lane = lax.broadcasted_iota(jnp.int32, (1, 128), 1)

    def by_element(ref, f, edge):
        v = jnp.zeros((1, 128), jnp.float32)
        for h in range(8):
            at = (lane >= edge * h) & (lane < edge * h + edge)
            v = jnp.where(at, ref[f, h], v)
        return v

    def fill_face(rnd, c, src):
        for k, y in enumerate((0, 15, 16, 31)):
            face[rnd, c, 16 * k : 16 * k + 8, :] = src[c, pl.ds(y, 8, stride=32), :]
            for x in range(8):
                at = 32 * (15 - x) + y
                face[rnd, c, 16 * k + 8 + x : 16 * k + 9 + x, :] = src[c, at : at + 1, :]
        face[rnd, c, X_FIRST : X_FIRST + 32, :] = src[c, 0:32]
        face[rnd, c, X_LAST : X_LAST + 32, :] = src[c, 480:512]

    def fill_corner(full, rnd, c):
        for k, at in enumerate((X_FIRST, X_FIRST + 31, X_LAST, X_LAST + 31)):
            corner[full, k, c] = face[rnd, c, at : at + 1, :]

    def z_forward(x):
        hi, lo = halves(x)
        return dot(jnp.concatenate([hi, lo, hi], axis=1), zf[...])

    def face_ends(rnd, c):
        hi, lo = halves(face[rnd, c])
        return dot(jnp.concatenate([hi, lo], axis=1), zf[:256, 128:])

    def gather_ends(ends, edge):
        total = ends[0]
        for k in range(1, 4):
            total = total + pltpu.roll(ends[k], k, 1)
        total = jnp.where(lane < HIGH + 4, total, pltpu.roll(edge, 16, 1))
        t = jnp.transpose(total)
        return t[LOW : LOW + 4], t[HIGH : HIGH + 4], t[LOW + 16 : LOW + 17], t[HIGH + 16 : HIGH + 17]

    def put_ends(rnd, c, low, high, edge_low, edge_high):
        for s, (planes, edge) in enumerate(((low, edge_low), (high, edge_high))):
            zsend[rnd, s, c, 0:4] = planes
            zsend[rnd, s, c, 4:5] = edge
            if rnd != 1:
                zedge[0 if rnd == 0 else 1, s, c] = edge

    def main_part(c, src):
        parts = []
        for f in range(2):
            near = [src[c, 32 * x + 16 * f : 32 * x + 16 * f + 16] for x in range(8)]
            far = [src[c, 32 * (15 - x) + 16 * f : 32 * (15 - x) + 16 * f + 16] for x in range(8)]
            parts += [n + m for n, m in zip(near, far)] + [n - m for n, m in zip(near, far)]
        m = z_forward(jnp.concatenate(parts, axis=0))
        ends = []
        for k in range(4):
            hi, lo = halves(m[128 * k : 128 * k + 128, :128])
            part_hi[c, k] = hi
            part_lo[c, k] = lo
            end = m[128 * k : 128 * k + 128, 128:]
            part_end[c, k] = end
            ends.append(end)
        return ends

    def ring_part(c, rnd, full):
        xm, xp = rx[rnd, 1, c], rx[rnd, 0, c]
        sums = (xm + xp, xm - xp)
        for p in range(2):
            fold = (lambda a, b: a + b) if p == 0 else (lambda a, b: a - b)
            ring[p, 0:16] = sums[p][0:16]
            ring[2 + p, 0:16] = sums[p][16:32]
            ym, yp = ry[rnd, 1, c], ry[rnd, 0, c]
            mid = face[rnd, c, Y_MID : Y_MID + 32]
            ring[p, 16:24] = fold(ym[0:8], ym[8:16])
            ring[p, 24:32] = fold(mid[16:24], mid[24:32])
            ring[2 + p, 16:24] = fold(mid[0:8], mid[8:16])
            ring[2 + p, 24:32] = fold(yp[0:8], yp[8:16])
            ring[p, 32:33] = fold(rc[full, 3, c], rc[full, 1, c])
            ring[p, 33:34] = sums[p][16:17]
            ring[2 + p, 32:33] = sums[p][15:16]
            ring[2 + p, 33:34] = fold(rc[full, 2, c], rc[full, 0, c])
        return z_forward(ring[...].reshape(4 * RING, 128))

    def ring_planes(c, full, rnd):
        rows = []
        for s in (1, 0):
            got = lambda dx, dy: re[full, s, slot((dx, dy)), c]
            own = rz[rnd, s, c, 4:5]
            t = jnp.where((lane >= 48) & (lane < 64), got(0, 1), own)
            t = jnp.where((lane >= 64) & (lane < 95), got(-1, 0), t)
            t = jnp.where(lane == 95, got(-1, 1), t)
            t = jnp.where((lane >= 96) & (lane < 127), got(1, 0), t)
            t = jnp.where(lane == 127, got(1, 1), t)
            rows += [t, t]
            t = jnp.where(lane < 16, got(0, -1), own)
            t = jnp.where(lane == 64, got(-1, -1), t)
            t = jnp.where((lane > 64) & (lane < 96), got(-1, 0), t)
            t = jnp.where(lane == 96, got(1, -1), t)
            t = jnp.where(lane > 96, got(1, 0), t)
            rows += [t, t]
        t = jnp.concatenate([jnp.zeros((56, 128), jnp.float32)] + rows + [jnp.zeros((64, 128), jnp.float32)], axis=0)
        t = jnp.transpose(t)
        for p in range(2):
            fold = (lambda a, b: a + b) if p == 0 else (lambda a, b: a - b)
            ends = fold(t[96:128], t[64:96])
            ring_end[p, 0:16] = ends[0:16]
            ring_end[2 + p, 0:16] = ends[16:32]
            ring_end[p, 16:24] = fold(t[48:56], t[56:64])
            ring_end[p, 24:32] = fold(t[32:40], t[40:48])
            ring_end[2 + p, 16:24] = fold(t[16:24], t[24:32])
            ring_end[2 + p, 24:32] = fold(t[0:8], t[8:16])
            ring_end[p, 32:33] = ends[31:32]
            ring_end[p, 33:34] = ends[16:17]
            ring_end[2 + p, 32:33] = ends[15:16]
            ring_end[2 + p, 33:34] = ends[0:1]

    def solve(c, rnd, full, inner):
        around = ring_part(c, rnd, full)
        ring_planes(c, full, rnd)
        blank = jnp.zeros((56, 128), jnp.float32)
        planes = [blank, rz[rnd, 1, c, 0:4], rz[rnd, 0, c, 0:4]]
        planes += [blank, jnp.zeros((8, 128), jnp.float32)] if inner is None else [inner, blank]
        planes = jnp.transpose(jnp.concatenate(planes, axis=0))
        outs = []
        for k in range(4):
            f, p = k // 2, k % 2
            eh, el = halves(jnp.where(lane < 48, part_end[c, k], planes))
            hi = jnp.concatenate([part_hi[c, k], eh], axis=1)
            lo = jnp.concatenate([part_lo[c, k], el], axis=1)
            r = around[RING * k : RING * k + RING]
            r = jnp.concatenate([r[:, :128], jnp.where(lane < 48, r[:, 128:], ring_end[k])], axis=1)
            rh, rl = wide_halves(r)
            r = jnp.concatenate([rh, rl, rh, jnp.zeros((8, 256), jnp.float32)], axis=0).astype(jnp.bfloat16)
            m = dot(into[p], jnp.concatenate([hi, lo, hi, r], axis=0))[:HALF]
            t = m + m[:, 128 + LOW + k : 129 + LOW + k] * row[0:1]
            t = t + m[:, 128 + HIGH + k : 129 + HIGH + k] * row[1:2]
            if inner is not None:
                t = t + m[:, 136 + LOW + k : 137 + LOW + k] * row[2:3]
                t = t + m[:, 136 + HIGH + k : 137 + HIGH + k] * row[3:4]
            th, tl = wide_halves(t * inv[k])
            data = jnp.concatenate([th, tl, th, jnp.zeros((8, 256), jnp.float32)], axis=0).astype(jnp.bfloat16)
            u = dot(outof[p], data)
            hi, lo = halves(u[:, :128])
            eh, el = wide_halves(u[:, 128:])
            end = jnp.where((lane >= 16) & (lane < 32), el, eh).astype(jnp.bfloat16)
            outs.append(jnp.concatenate([hi, lo, hi, end], axis=1))
        return jnp.concatenate(outs, axis=0)

    def unfold(x, put):
        for f in range(2):
            for i in range(8):
                s = x[256 * f + 16 * i : 256 * f + 16 * i + 16, :128]
                d = x[256 * f + 128 + 16 * i : 256 * f + 128 + 16 * i + 16, :128]
                put(32 * i + 16 * f, s + d)
                put(32 * (15 - i) + 16 * f, s - d)

    for c in range(3):
        loads[c].wait()
        fill_face(0, c, rhs)
        fill_corner(0, 0, c)
    loads[3].wait()
    for c in range(3):
        ends = main_part(c, rhs)
        put_ends(0, c, *gather_ends(ends, face_ends(0, c)))
    pl.semaphore_wait(barrier, count)
    for c in range(3):
        send(0, c, lambda d: True)
    for k in range(4, 11):
        loads[k].wait()

    for f in range(2):
        for t in range(2):
            part = slice(128 * t, 128 * t + 128)
            if t == 0:
                v, r = by_element(visc_ref, f, SPAN), by_element(reac_ref, f, SPAN)
                v = jnp.where(lane >= 7 * SPAN, visc_ref[f, 7], v)
                r = jnp.where(lane >= 7 * SPAN, reac_ref[f, 7], r)
            else:
                v, r = jnp.full((1, 128), visc_ref[f, 7]), jnp.full((1, 128), reac_ref[f, 7])
            for p in range(2):
                inv[2 * f + p, :, part] = 1.0 / (v * (lam[p] + row[4:5, part]) + r)
        v, r = by_element(visc_ref, f, EDGE), by_element(reac_ref, f, EDGE)
        visc_plane[16 * f : 16 * f + 16] = jnp.broadcast_to(v, (16, 128))
        coef_plane[16 * f : 16 * f + 16] = jnp.broadcast_to(r + 6.0 * v, (16, 128))

    part_row = lax.broadcasted_iota(jnp.int32, (4, 128), 0)
    upper = ((lane >= 32) & (lane < 64)) | ((lane >= 80) & (lane < 96)) | (lane >= 112)
    plane_visc = [jnp.where(part_row < 2, visc_ref[0, h], visc_ref[1, h]) for h in (0, 7)]
    edge_visc = [jnp.where(upper, visc_ref[1, h], visc_ref[0, h]) for h in (0, 7)]

    for c in range(3):
        arrive(0, c)
        lhs = solve(c, 0, 0, None)
        x = dot(lhs, zb[...])

        def put_first(at, v, c=c):
            first[c, at : at + 16] = v

        unfold(x, put_first)
        fill_face(1, c, first)
        send(1, c, flat)
        ends = [x[128 * k : 128 * k + 128, 128:] for k in range(4)]
        put_ends(1, c, *gather_ends(ends, face_ends(1, c)))
        send(1, c, deep)

    y_index = lax.broadcasted_iota(jnp.int32, (32, 128), 0)
    inner = []
    for c in range(3):
        arrive(1, c)
        for x in range(16):
            v = first[c, 32 * x : 32 * x + 32]
            beside = rx[1, 1, c] if x == 0 else first[c, 32 * x - 32 : 32 * x]
            beside = beside + (rx[1, 0, c] if x == 15 else first[c, 32 * x + 32 : 32 * x + 64])
            at = x if x < 8 else 23 - x
            ylo, yhi = ry[1, 1, c, at : at + 1], ry[1, 0, c, at : at + 1]
            beside = beside + jnp.where(y_index == 0, ylo, pltpu.roll(v, 1, 0))
            beside = beside + jnp.where(y_index == 31, yhi, pltpu.roll(v, 31, 0))
            beside = beside + jnp.where(lane == 0, 0.0, pltpu.roll(v, 1, 1))
            beside = beside + jnp.where(lane == 127, 0.0, pltpu.roll(v, 127, 1))
            resid[c, 32 * x : 32 * x + 32] = (
                rhs[c, 32 * x : 32 * x + 32] - coef_plane[...] * v + visc_plane[...] * beside
            )
        fill_face(2, c, resid)
        planes = [plane_visc[s] * rz[1, 1 - s, c, 0:4] for s in range(2)]
        edge = [edge_visc[s] * rz[1, 1 - s, c, 4:5] for s in range(2)]
        inner.append(jnp.concatenate(planes, axis=0))
        face_low_high = face_ends(2, c)
        add = jnp.transpose(
            jnp.concatenate([edge[0], jnp.zeros((126, 128), jnp.float32), edge[1]], axis=0)
        )
        face[2, c] = face[2, c] + add
        fill_corner(1, 2, c)
        send(2, c, flat)
        ends = main_part(c, resid)
        low, high, edge_low, edge_high = gather_ends(ends, face_low_high)
        put_ends(2, c, low + planes[0], high + planes[1], edge_low + edge[0], edge_high + edge[1])
        send(2, c, deep)

    for c in range(3):
        arrive(2, c)
        lhs = solve(c, 2, 1, inner[c])
        x = dot(lhs, zb[:, :128])

        def put_last(at, v, c=c):
            out_ref[c, at : at + 16] = first[c, at : at + 16] + v

        unfold(x, put_last)

    for (rnd, c, d), copy in copies.items():
        pl.when(exists(d))(copy.wait_send)


def shards(sizes, rhs, viscous, reaction):
    f32, bf16 = jnp.float32, jnp.bfloat16
    consts = constants()
    any_space = pl.BlockSpec(memory_space=pl.ANY)
    vmem = pl.BlockSpec(memory_space=pltpu.VMEM)
    copies = 3 * (2 * len(DIRS) + len(FACES))
    scratch = [
        pltpu.VMEM((3, 512, 128), f32),
        pltpu.VMEM((3, 512, 128), f32),
        pltpu.VMEM((3, 512, 128), f32),
        pltpu.VMEM((3, 3, 128, 128), f32),
        pltpu.VMEM((2, 4, 3, 1, 128), f32),
        pltpu.VMEM((3, 2, 3, 8, 128), f32),
        pltpu.VMEM((2, 2, 3, 1, 128), f32),
        pltpu.VMEM((3, 2, 3, 32, 128), f32),
        pltpu.VMEM((3, 2, 3, 16, 128), f32),
        pltpu.VMEM((2, 4, 3, 1, 128), f32),
        pltpu.VMEM((3, 2, 3, 8, 128), f32),
        pltpu.VMEM((2, 2, 9, 3, 1, 128), f32),
        pltpu.VMEM((3, 4, 128, 128), bf16),
        pltpu.VMEM((3, 4, 128, 128), bf16),
        pltpu.VMEM((3, 4, 128, 128), f32),
        pltpu.VMEM((4, RING, 128), f32),
        pltpu.VMEM((4, RING, 128), f32),
        pltpu.VMEM((4, HALF, 256), f32),
        pltpu.VMEM((32, 128), f32),
        pltpu.VMEM((32, 128), f32),
    ]
    scratch += [pltpu.VMEM(t.shape, t.dtype) for t in consts]
    scratch += [
        pltpu.SMEM((2, 8), f32),
        pltpu.SMEM((2, 8), f32),
        pltpu.SemaphoreType.DMA((11,)),
        pltpu.SemaphoreType.DMA((copies,)),
        pltpu.SemaphoreType.DMA((copies,)),
    ]
    operands = (rhs.reshape(3, 512, 128), viscous.reshape(2, 8), reaction.reshape(2, 8), *consts)
    out = pl.pallas_call(
        functools.partial(kernel, sizes),
        out_shape=jax.ShapeDtypeStruct((3, 512, 128), f32),
        in_specs=[any_space] * len(operands),
        out_specs=vmem,
        scratch_shapes=scratch,
        compiler_params=pltpu.CompilerParams(
            collective_id=0, has_side_effects=True, vmem_limit_bytes=40 * 2**20
        ),
    )(*[pltpu.with_memory_space_constraint(jnp.asarray(a), pltpu.HBM) for a in operands])
    return out.reshape(rhs.shape)


def solution(mesh):
    sizes = tuple(mesh.shape[a] for a in ("gx", "gy", "gz"))
    placed = (P(None, "gx", "gy", "gz"), P("gx", "gy", "gz"), P("gx", "gy", "gz"))
    return jax.shard_map(
        functools.partial(shards, sizes),
        mesh=mesh,
        in_specs=placed,
        out_specs=P(None, "gx", "gy", "gz"),
        check_vma=False,
    )
```

```python
import functools

import jax
import jax.numpy as jnp
import numpy as np
from jax import lax
from jax.experimental import pallas as pl
from jax.experimental.pallas import tpu as pltpu
from jax.sharding import PartitionSpec as P

EDGE = 16
SPAN = EDGE + 2
HALF = 168
RING = 40
LOW, HIGH = 56, 60
MESH = pl.DeviceIdType.MESH
NN = (((1,), (0,)), ((), ()))
DIRS = [
    (dx, dy, dz)
    for dz in (0, -1, 1)
    for dy in (0, -1, 1)
    for dx in (0, -1, 1)
    if (dx, dy, dz) != (0, 0, 0)
]
FACES = [d for d in DIRS if sum(map(abs, d)) == 1]
Y_FIRST, Y_MID, Y_LAST, X_FIRST, X_LAST = 0, 16, 48, 64, 96


def table_halves(x):
    x = x.astype(np.float32)
    hi = x.astype(jnp.bfloat16)
    return hi, (x - hi.astype(np.float32)).astype(jnp.bfloat16)


def constants():
    i = np.arange(SPAN)
    basis = np.sqrt(2.0 / (SPAN + 1)) * np.sin(np.pi * np.outer(i + 1, i + 1) / (SPAN + 1))
    lam = 2.0 - 2.0 * np.cos(np.pi * (i + 1) / (SPAN + 1))
    q = np.arange(144)
    lanes = np.concatenate([np.arange(128), np.tile(np.arange(128, 144), 3)])
    forward = np.zeros((128, 256))
    back = np.zeros((144, 128))
    for h in range(8):
        for z in range(128):
            w = z - EDGE * h + 1
            if 0 <= w < SPAN:
                for n, k in enumerate(lanes):
                    if k // SPAN == h:
                        forward[z, n] = basis[w, k % SPAN]
            if 1 <= w <= EDGE:
                back[h * SPAN : (h + 1) * SPAN, z] = basis[w]
    forward[0, 128 + LOW] = 1.0
    forward[127, 128 + HIGH] = 1.0
    wide = np.zeros((144, 256))
    wide[:, :128] = back
    wide[:, 128 + LOW] = 2.0 * back[:, 0]
    wide[:, 128 + HIGH] = 2.0 * back[:, 127]
    fh, fl = table_halves(forward)
    bh, bl = table_halves(wide)
    z_forward = np.concatenate([fh, fh, fl], axis=0)
    z_back = np.concatenate(
        [bh[:128], bh[:128], bl[:128], bh[128:], bh[128:], bl[128:], np.zeros((80, 256), bh.dtype)], axis=0
    )
    into, out_of, lam_xy = [], [], []
    for parity in range(2):
        mode = np.arange(162)
        a, b = 2 * (mode // SPAN) + parity, mode % SPAN
        point = lambda x, y: basis[x, a] * basis[y, b]
        main = np.zeros((176, 128))
        for x in range(8):
            for y in range(16):
                main[:162, 16 * x + y] = point(x + 1, y + 1)
        ring = np.zeros((176, RING))
        for y in range(16):
            ring[:162, y] = point(0, y + 1)
        for x in range(8):
            ring[:162, 16 + x] = point(x + 1, 0)
            ring[:162, 24 + x] = point(x + 1, 17)
        ring[:162, 32], ring[:162, 33] = point(0, 0), point(0, 17)
        mh, ml = table_halves(main)
        rh, rl = table_halves(ring)
        into.append(np.concatenate([mh, mh, ml, rh, rh, rl, np.zeros((176, 8), mh.dtype)], axis=1))
        th, tl = mh[:HALF].T, ml[:HALF].T
        out_of.append(np.concatenate([th, th, tl, np.zeros((128, 8), mh.dtype)], axis=1))
        col = np.zeros((HALF, 1))
        col[:162, 0] = lam[a] + lam[b]
        lam_xy.append(np.repeat(col, 128, 1))
    rows = np.zeros((8, 256))
    for n, k in enumerate(lanes):
        if k < SPAN:
            rows[0, n], rows[2, n] = basis[0, k], basis[1, k]
        if k >= 7 * SPAN:
            rows[1, n], rows[3, n] = basis[17, k % SPAN], basis[16, k % SPAN]
        rows[4, n] = lam[k % SPAN]
    f32 = functools.partial(np.asarray, dtype=np.float32)
    return z_forward, np.stack(into), np.stack(out_of), z_back, f32(rows), f32(np.stack(lam_xy))


def dot(a, b):
    return lax.dot_general(a, b, NN, preferred_element_type=jnp.float32)


def halves(x):
    hi = x.astype(jnp.bfloat16)
    return hi, (x - hi.astype(jnp.float32)).astype(jnp.bfloat16)


def wide_halves(x):
    hi = x.astype(jnp.bfloat16).astype(jnp.float32)
    return hi, x - hi


def kernel(
    sizes, rhs_hbm, visc_hbm, reac_hbm, zf_hbm, into_hbm, outof_hbm, zb_hbm, row_hbm, lam_hbm,
    out_ref,
    rhs, first, resid, face, corner, zsend, zedge, rx, ry, rc, rz, re,
    part_hi, part_lo, part_end, ring, ring_end, inv, visc_plane, coef_plane,
    zf, into, outof, zb, row, lam, visc_ref, reac_ref, load_sem, send_sem, recv_sem,
):
    me = tuple(lax.axis_index(a) for a in ("gx", "gy", "gz"))

    def exists(d):
        ok = None
        for p, n, s in zip(me, sizes, d):
            if s:
                c = (p + s >= 0) & (p + s < n)
                ok = c if ok is None else ok & c
        return ok

    def peer(d):
        return tuple(p + s for p, s in zip(me, d))

    def minus(d):
        return tuple(-s for s in d)

    barrier = pltpu.get_barrier_semaphore()
    count = jnp.int32(0)
    for d in DIRS:
        ok = exists(d)
        count = count + ok.astype(jnp.int32)

        @pl.when(ok)
        def _(d=d):
            pl.semaphore_signal(barrier, inc=1, device_id=peer(d), device_id_type=MESH)

    loads = []
    pairs = [(rhs_hbm.at[c], rhs.at[c]) for c in range(3)]
    pairs += [(zf_hbm, zf), (visc_hbm, visc_ref), (reac_hbm, reac_ref), (row_hbm, row), (lam_hbm, lam), (into_hbm, into), (outof_hbm, outof), (zb_hbm, zb)]
    for k, (src, dst) in enumerate(pairs):
        loads.append(pltpu.make_async_copy(src, dst, load_sem.at[k]))
        loads[-1].start()

    def pieces(rnd, c, d):
        dx, dy, dz = d
        full = 0 if rnd == 0 else 1
        if dz == 0 and dy == 0:
            return face.at[rnd, c, pl.ds(X_LAST if dx > 0 else X_FIRST, 32), :], rx.at[rnd, int(dx > 0), c]
        if dz == 0 and dx == 0:
            return face.at[rnd, c, pl.ds(Y_LAST if dy > 0 else Y_FIRST, 16), :], ry.at[rnd, int(dy > 0), c]
        if dz == 0:
            k = 2 * int(dx > 0) + int(dy > 0)
            return corner.at[full, k, c], rc.at[full, k, c]
        s = int(dz > 0)
        if dx == 0 and dy == 0:
            return zsend.at[rnd, s, c], rz.at[rnd, s, c]
        return zedge.at[full, s, c], re.at[full, s, slot(d), c]

    def slot(d):
        return 3 * (d[0] + 1) + d[1] + 1

    copies = {}
    for rnd in range(3):
        for c in range(3):
            for d in DIRS if rnd != 1 else FACES:
                k = len(copies)
                src, dst = pieces(rnd, c, d)
                copies[rnd, c, d] = pltpu.make_async_remote_copy(
                    src_ref=src, dst_ref=dst, send_sem=send_sem.at[k], recv_sem=recv_sem.at[k],
                    device_id=peer(d), device_id_type=MESH,
                )

    def send(rnd, c, ask):
        for (r, cc, d), copy in copies.items():
            if r == rnd and cc == c and ask(d):
                pl.when(exists(d))(copy.start)

    def arrive(rnd, c, ask=lambda d: True):
        for (r, cc, d), copy in copies.items():
            if r == rnd and cc == c and ask(d):
                pl.when(exists(minus(d)))(copy.wait_recv)

    flat = lambda d: d[2] == 0
    deep = lambda d: d[2] != 0

    for d in DIRS:
        @pl.when(jnp.logical_not(exists(minus(d))))
        def _(d=d):
            for rnd in range(3):
                if rnd != 1 or d in FACES:
                    for c in range(3):
                        dst = pieces(rnd, c, d)[1]
                        dst[...] = jnp.zeros(dst.shape, jnp.float32)

    zsend[...] = jnp.zeros(zsend.shape, jnp.float32)
    for k in range(4):
        ring[k, 32:40] = jnp.zeros((8, 128), jnp.float32)
        ring_end[k, 32:40] = jnp.zeros((8, 128), jnp.float32)

    lane = lax.broadcasted_iota(jnp.int32, (1, 128), 1)

    def by_element(ref, f, edge):
        v = jnp.zeros((1, 128), jnp.float32)
        for h in range(8):
            at = (lane >= edge * h) & (lane < edge * h + edge)
            v = jnp.where(at, ref[f, h], v)
        return v

    def fill_face(rnd, c, src):
        for k, y in enumerate((0, 15, 16, 31)):
            face[rnd, c, 16 * k : 16 * k + 8, :] = src[c, pl.ds(y, 8, stride=32), :]
            for x in range(8):
                at = 32 * (15 - x) + y
                face[rnd, c, 16 * k + 8 + x : 16 * k + 9 + x, :] = src[c, at : at + 1, :]
        face[rnd, c, X_FIRST : X_FIRST + 32, :] = src[c, 0:32]
        face[rnd, c, X_LAST : X_LAST + 32, :] = src[c, 480:512]

    def fill_corner(full, rnd, c):
        for k, at in enumerate((X_FIRST, X_FIRST + 31, X_LAST, X_LAST + 31)):
            corner[full, k, c] = face[rnd, c, at : at + 1, :]

    def z_forward(x):
        hi, lo = halves(x)
        return dot(jnp.concatenate([hi, lo, hi], axis=1), zf[...])

    def face_ends(rnd, c):
        hi, lo = halves(face[rnd, c])
        return dot(jnp.concatenate([hi, lo], axis=1), zf[:256, 128:])

    def gather_ends(ends, edge):
        total = ends[0]
        for k in range(1, 4):
            total = total + pltpu.roll(ends[k], k, 1)
        total = jnp.where(lane < HIGH + 4, total, pltpu.roll(edge, 16, 1))
        t = jnp.transpose(total)
        return t[LOW : LOW + 4], t[HIGH : HIGH + 4], t[LOW + 16 : LOW + 17], t[HIGH + 16 : HIGH + 17]

    def put_ends(rnd, c, low, high, edge_low, edge_high):
        for s, (planes, edge) in enumerate(((low, edge_low), (high, edge_high))):
            zsend[rnd, s, c, 0:4] = planes
            zsend[rnd, s, c, 4:5] = edge
            if rnd != 1:
                zedge[0 if rnd == 0 else 1, s, c] = edge

    def main_part(c, src):
        parts = []
        for f in range(2):
            near = [src[c, 32 * x + 16 * f : 32 * x + 16 * f + 16] for x in range(8)]
            far = [src[c, 32 * (15 - x) + 16 * f : 32 * (15 - x) + 16 * f + 16] for x in range(8)]
            parts += [n + m for n, m in zip(near, far)] + [n - m for n, m in zip(near, far)]
        m = z_forward(jnp.concatenate(parts, axis=0))
        ends = []
        for k in range(4):
            hi, lo = halves(m[128 * k : 128 * k + 128, :128])
            part_hi[c, k] = hi
            part_lo[c, k] = lo
            end = m[128 * k : 128 * k + 128, 128:]
            part_end[c, k] = end
            ends.append(end)
        return ends

    def ring_part(c, rnd, full):
        xm, xp = rx[rnd, 1, c], rx[rnd, 0, c]
        sums = (xm + xp, xm - xp)
        for p in range(2):
            fold = (lambda a, b: a + b) if p == 0 else (lambda a, b: a - b)
            ring[p, 0:16] = sums[p][0:16]
            ring[2 + p, 0:16] = sums[p][16:32]
            ym, yp = ry[rnd, 1, c], ry[rnd, 0, c]
            mid = face[rnd, c, Y_MID : Y_MID + 32]
            ring[p, 16:24] = fold(ym[0:8], ym[8:16])
            ring[p, 24:32] = fold(mid[16:24], mid[24:32])
            ring[2 + p, 16:24] = fold(mid[0:8], mid[8:16])
            ring[2 + p, 24:32] = fold(yp[0:8], yp[8:16])
            ring[p, 32:33] = fold(rc[full, 3, c], rc[full, 1, c])
            ring[p, 33:34] = sums[p][16:17]
            ring[2 + p, 32:33] = sums[p][15:16]
            ring[2 + p, 33:34] = fold(rc[full, 2, c], rc[full, 0, c])
        return z_forward(ring[...].reshape(4 * RING, 128))

    def ring_planes(c, full, rnd):
        rows = []
        for s in (1, 0):
            got = lambda dx, dy: re[full, s, slot((dx, dy)), c]
            own = rz[rnd, s, c, 4:5]
            t = jnp.where((lane >= 48) & (lane < 64), got(0, 1), own)
            t = jnp.where((lane >= 64) & (lane < 95), got(-1, 0), t)
            t = jnp.where(lane == 95, got(-1, 1), t)
            t = jnp.where((lane >= 96) & (lane < 127), got(1, 0), t)
            t = jnp.where(lane == 127, got(1, 1), t)
            rows += [t, t]
            t = jnp.where(lane < 16, got(0, -1), own)
            t = jnp.where(lane == 64, got(-1, -1), t)
            t = jnp.where((lane > 64) & (lane < 96), got(-1, 0), t)
            t = jnp.where(lane == 96, got(1, -1), t)
            t = jnp.where(lane > 96, got(1, 0), t)
            rows += [t, t]
        t = jnp.concatenate([jnp.zeros((56, 128), jnp.float32)] + rows + [jnp.zeros((64, 128), jnp.float32)], axis=0)
        t = jnp.transpose(t)
        for p in range(2):
            fold = (lambda a, b: a + b) if p == 0 else (lambda a, b: a - b)
            ends = fold(t[96:128], t[64:96])
            ring_end[p, 0:16] = ends[0:16]
            ring_end[2 + p, 0:16] = ends[16:32]
            ring_end[p, 16:24] = fold(t[48:56], t[56:64])
            ring_end[p, 24:32] = fold(t[32:40], t[40:48])
            ring_end[2 + p, 16:24] = fold(t[16:24], t[24:32])
            ring_end[2 + p, 24:32] = fold(t[0:8], t[8:16])
            ring_end[p, 32:33] = ends[31:32]
            ring_end[p, 33:34] = ends[16:17]
            ring_end[2 + p, 32:33] = ends[15:16]
            ring_end[2 + p, 33:34] = ends[0:1]

    def solve(c, rnd, full, inner):
        around = ring_part(c, rnd, full)
        ring_planes(c, full, rnd)
        blank = jnp.zeros((56, 128), jnp.float32)
        planes = [blank, rz[rnd, 1, c, 0:4], rz[rnd, 0, c, 0:4]]
        planes += [blank, jnp.zeros((8, 128), jnp.float32)] if inner is None else [inner, blank]
        planes = jnp.transpose(jnp.concatenate(planes, axis=0))
        ms = []
        for k in range(4):
            eh, el = halves(jnp.where(lane < 48, part_end[c, k], planes))
            hi = jnp.concatenate([part_hi[c, k], eh], axis=1)
            lo = jnp.concatenate([part_lo[c, k], el], axis=1)
            r = around[RING * k : RING * k + RING]
            r = jnp.concatenate([r[:, :128], jnp.where(lane < 48, r[:, 128:], ring_end[k])], axis=1)
            rh, rl = wide_halves(r)
            r = jnp.concatenate([rh, rl, rh, jnp.zeros((8, 256), jnp.float32)], axis=0).astype(jnp.bfloat16)
            ms.append(dot(into[k % 2], jnp.concatenate([hi, lo, hi, r], axis=0))[:HALF])
        us = []
        for k in range(4):
            m = ms[k]
            t = m + m[:, 128 + LOW + k : 129 + LOW + k] * row[0:1]
            t = t + m[:, 128 + HIGH + k : 129 + HIGH + k] * row[1:2]
            if inner is not None:
                t = t + m[:, 136 + LOW + k : 137 + LOW + k] * row[2:3]
                t = t + m[:, 136 + HIGH + k : 137 + HIGH + k] * row[3:4]
            th, tl = wide_halves(t * inv[k])
            data = jnp.concatenate([th, tl, th, jnp.zeros((8, 256), jnp.float32)], axis=0).astype(jnp.bfloat16)
            us.append(dot(outof[k % 2], data))
        outs = []
        for u in us:
            hi, lo = halves(u[:, :128])
            eh, el = wide_halves(u[:, 128:])
            end = jnp.where((lane >= 16) & (lane < 32), el, eh).astype(jnp.bfloat16)
            outs.append(jnp.concatenate([hi, lo, hi, end], axis=1))
        return jnp.concatenate(outs, axis=0)

    def unfold(x, put):
        for f in range(2):
            for i in range(8):
                s = x[256 * f + 16 * i : 256 * f + 16 * i + 16, :128]
                d = x[256 * f + 128 + 16 * i : 256 * f + 128 + 16 * i + 16, :128]
                put(32 * i + 16 * f, s + d)
                put(32 * (15 - i) + 16 * f, s - d)

    for c in range(3):
        loads[c].wait()
        fill_face(0, c, rhs)
        fill_corner(0, 0, c)
    loads[3].wait()
    for c in range(3):
        ends = main_part(c, rhs)
        put_ends(0, c, *gather_ends(ends, face_ends(0, c)))
    pl.semaphore_wait(barrier, count)
    for c in range(3):
        send(0, c, lambda d: True)
    for k in range(4, 11):
        loads[k].wait()

    for f in range(2):
        for t in range(2):
            part = slice(128 * t, 128 * t + 128)
            if t == 0:
                v, r = by_element(visc_ref, f, SPAN), by_element(reac_ref, f, SPAN)
                v = jnp.where(lane >= 7 * SPAN, visc_ref[f, 7], v)
                r = jnp.where(lane >= 7 * SPAN, reac_ref[f, 7], r)
            else:
                v, r = jnp.full((1, 128), visc_ref[f, 7]), jnp.full((1, 128), reac_ref[f, 7])
            for p in range(2):
                inv[2 * f + p, :, part] = 1.0 / (v * (lam[p] + row[4:5, part]) + r)
        v, r = by_element(visc_ref, f, EDGE), by_element(reac_ref, f, EDGE)
        visc_plane[16 * f : 16 * f + 16] = jnp.broadcast_to(v, (16, 128))
        coef_plane[16 * f : 16 * f + 16] = jnp.broadcast_to(r + 6.0 * v, (16, 128))

    part_row = lax.broadcasted_iota(jnp.int32, (4, 128), 0)
    upper = ((lane >= 32) & (lane < 64)) | ((lane >= 80) & (lane < 96)) | (lane >= 112)
    plane_visc = [jnp.where(part_row < 2, visc_ref[0, h], visc_ref[1, h]) for h in (0, 7)]
    edge_visc = [jnp.where(upper, visc_ref[1, h], visc_ref[0, h]) for h in (0, 7)]

    for c in range(3):
        arrive(0, c)
        lhs = solve(c, 0, 0, None)
        x = dot(lhs, zb[...])

        def put_first(at, v, c=c):
            first[c, at : at + 16] = v

        unfold(x, put_first)
        fill_face(1, c, first)
        send(1, c, flat)
        ends = [x[128 * k : 128 * k + 128, 128:] for k in range(4)]
        put_ends(1, c, *gather_ends(ends, face_ends(1, c)))
        send(1, c, deep)

    y_index = lax.broadcasted_iota(jnp.int32, (32, 128), 0)
    inner = []
    for c in range(3):
        arrive(1, c)
        for x in range(16):
            v = first[c, 32 * x : 32 * x + 32]
            beside = rx[1, 1, c] if x == 0 else first[c, 32 * x - 32 : 32 * x]
            beside = beside + (rx[1, 0, c] if x == 15 else first[c, 32 * x + 32 : 32 * x + 64])
            at = x if x < 8 else 23 - x
            ylo, yhi = ry[1, 1, c, at : at + 1], ry[1, 0, c, at : at + 1]
            beside = beside + jnp.where(y_index == 0, ylo, pltpu.roll(v, 1, 0))
            beside = beside + jnp.where(y_index == 31, yhi, pltpu.roll(v, 31, 0))
            beside = beside + jnp.where(lane == 0, 0.0, pltpu.roll(v, 1, 1))
            beside = beside + jnp.where(lane == 127, 0.0, pltpu.roll(v, 127, 1))
            resid[c, 32 * x : 32 * x + 32] = (
                rhs[c, 32 * x : 32 * x + 32] - coef_plane[...] * v + visc_plane[...] * beside
            )
        fill_face(2, c, resid)
        planes = [plane_visc[s] * rz[1, 1 - s, c, 0:4] for s in range(2)]
        edge = [edge_visc[s] * rz[1, 1 - s, c, 4:5] for s in range(2)]
        inner.append(jnp.concatenate(planes, axis=0))
        face_low_high = face_ends(2, c)
        add = jnp.transpose(
            jnp.concatenate([edge[0], jnp.zeros((126, 128), jnp.float32), edge[1]], axis=0)
        )
        face[2, c] = face[2, c] + add
        fill_corner(1, 2, c)
        send(2, c, flat)
        ends = main_part(c, resid)
        low, high, edge_low, edge_high = gather_ends(ends, face_low_high)
        put_ends(2, c, low + planes[0], high + planes[1], edge_low + edge[0], edge_high + edge[1])
        send(2, c, deep)

    for c in range(3):
        arrive(2, c)
        lhs = solve(c, 2, 1, inner[c])
        x = dot(lhs, zb[:, :128])

        def put_last(at, v, c=c):
            out_ref[c, at : at + 16] = first[c, at : at + 16] + v

        unfold(x, put_last)

    for (rnd, c, d), copy in copies.items():
        pl.when(exists(d))(copy.wait_send)


def shards(sizes, rhs, viscous, reaction):
    f32, bf16 = jnp.float32, jnp.bfloat16
    consts = constants()
    any_space = pl.BlockSpec(memory_space=pl.ANY)
    vmem = pl.BlockSpec(memory_space=pltpu.VMEM)
    copies = 3 * (2 * len(DIRS) + len(FACES))
    scratch = [
        pltpu.VMEM((3, 512, 128), f32),
        pltpu.VMEM((3, 512, 128), f32),
        pltpu.VMEM((3, 512, 128), f32),
        pltpu.VMEM((3, 3, 128, 128), f32),
        pltpu.VMEM((2, 4, 3, 1, 128), f32),
        pltpu.VMEM((3, 2, 3, 8, 128), f32),
        pltpu.VMEM((2, 2, 3, 1, 128), f32),
        pltpu.VMEM((3, 2, 3, 32, 128), f32),
        pltpu.VMEM((3, 2, 3, 16, 128), f32),
        pltpu.VMEM((2, 4, 3, 1, 128), f32),
        pltpu.VMEM((3, 2, 3, 8, 128), f32),
        pltpu.VMEM((2, 2, 9, 3, 1, 128), f32),
        pltpu.VMEM((3, 4, 128, 128), bf16),
        pltpu.VMEM((3, 4, 128, 128), bf16),
        pltpu.VMEM((3, 4, 128, 128), f32),
        pltpu.VMEM((4, RING, 128), f32),
        pltpu.VMEM((4, RING, 128), f32),
        pltpu.VMEM((4, HALF, 256), f32),
        pltpu.VMEM((32, 128), f32),
        pltpu.VMEM((32, 128), f32),
    ]
    scratch += [pltpu.VMEM(t.shape, t.dtype) for t in consts]
    scratch += [
        pltpu.SMEM((2, 8), f32),
        pltpu.SMEM((2, 8), f32),
        pltpu.SemaphoreType.DMA((11,)),
        pltpu.SemaphoreType.DMA((copies,)),
        pltpu.SemaphoreType.DMA((copies,)),
    ]
    operands = (rhs.reshape(3, 512, 128), viscous.reshape(2, 8), reaction.reshape(2, 8), *consts)
    out = pl.pallas_call(
        functools.partial(kernel, sizes),
        out_shape=jax.ShapeDtypeStruct((3, 512, 128), f32),
        in_specs=[any_space] * len(operands),
        out_specs=vmem,
        scratch_shapes=scratch,
        compiler_params=pltpu.CompilerParams(
            collective_id=0, has_side_effects=True, vmem_limit_bytes=40 * 2**20
        ),
    )(*[pltpu.with_memory_space_constraint(jnp.asarray(a), pltpu.HBM) for a in operands])
    return out.reshape(rhs.shape)


def solution(mesh):
    sizes = tuple(mesh.shape[a] for a in ("gx", "gy", "gz"))
    placed = (P(None, "gx", "gy", "gz"), P("gx", "gy", "gz"), P("gx", "gy", "gz"))
    return jax.shard_map(
        functools.partial(shards, sizes),
        mesh=mesh,
        in_specs=placed,
        out_specs=P(None, "gx", "gy", "gz"),
        check_vma=False,
    )
```

```python
import functools

import jax
import jax.numpy as jnp
import numpy as np
from jax import lax
from jax.experimental import pallas as pl
from jax.experimental.pallas import tpu as pltpu
from jax.sharding import PartitionSpec as P

EDGE = 16
SPAN = EDGE + 2
HALF = 168
RING = 40
TAIL = 3 * SPAN
LOW, HIGH = 64, 68
MESH = pl.DeviceIdType.MESH
NN = (((1,), (0,)), ((), ()))
DIRS = [
    (dx, dy, dz)
    for dz in (0, -1, 1)
    for dy in (0, -1, 1)
    for dx in (0, -1, 1)
    if (dx, dy, dz) != (0, 0, 0)
]
FACES = [d for d in DIRS if sum(map(abs, d)) == 1]
Y_FIRST, Y_MID, Y_LAST, X_FIRST, X_LAST = 0, 16, 48, 64, 96


def table_halves(x):
    x = x.astype(np.float32)
    hi = x.astype(jnp.bfloat16)
    return hi, (x - hi.astype(np.float32)).astype(jnp.bfloat16)


def constants():
    i = np.arange(SPAN)
    basis = np.sqrt(2.0 / (SPAN + 1)) * np.sin(np.pi * np.outer(i + 1, i + 1) / (SPAN + 1))
    lam = 2.0 - 2.0 * np.cos(np.pi * (i + 1) / (SPAN + 1))
    lanes = np.concatenate([np.arange(126), [-1, -1], np.tile(np.arange(126, 144), 3)])
    forward = np.zeros((128, 256))
    back = np.zeros((144, 128))
    for h in range(8):
        for z in range(128):
            w = z - EDGE * h + 1
            if 0 <= w < SPAN:
                for n, k in enumerate(lanes):
                    if k >= 0 and k // SPAN == h:
                        forward[z, n] = basis[w, k % SPAN]
            if 1 <= w <= EDGE:
                back[h * SPAN : (h + 1) * SPAN, z] = basis[w]
    forward[0, 128 + LOW] = 1.0
    forward[127, 128 + HIGH] = 1.0
    wide = np.zeros((144, 256))
    wide[:, :128] = back
    wide[:, 128 + LOW] = 2.0 * back[:, 0]
    wide[:, 128 + HIGH] = 2.0 * back[:, 127]
    fh, fl = table_halves(forward)
    bh, bl = table_halves(wide)
    z_forward = np.concatenate([fh, fh, fl], axis=0)
    pad = lambda n: np.zeros((n, 256), bh.dtype)
    z_back = np.concatenate(
        [bh[:126], pad(2), bh[:126], pad(2), bl[:126], pad(2), bh[126:], bh[126:], bl[126:], pad(74)], axis=0
    )
    into, out_of, lam_xy = [], [], []
    for parity in range(2):
        mode = np.arange(162)
        a, b = 2 * (mode // SPAN) + parity, mode % SPAN
        point = lambda x, y: basis[x, a] * basis[y, b]
        main = np.zeros((176, 128))
        for x in range(8):
            for y in range(16):
                main[:162, 16 * x + y] = point(x + 1, y + 1)
        ring = np.zeros((176, RING))
        for y in range(16):
            ring[:162, y] = point(0, y + 1)
        for x in range(8):
            ring[:162, 16 + x] = point(x + 1, 0)
            ring[:162, 24 + x] = point(x + 1, 17)
        ring[:162, 32], ring[:162, 33] = point(0, 0), point(0, 17)
        mh, ml = table_halves(main)
        rh, rl = table_halves(ring)
        into.append(np.concatenate([mh, mh, ml, rh, rh, rl, np.zeros((176, 8), mh.dtype)], axis=1))
        col = np.zeros((HALF, 1))
        col[:162, 0] = lam[a] + lam[b]
        th, tl = mh[:HALF].T, ml[:HALF].T
        a, b = slice(0, 128), slice(128, HALF)
        out_of.append(
            np.concatenate(
                [th[:, a], th[:, a], tl[:, a], th[:, b], th[:, b], tl[:, b], np.zeros((128, 8), mh.dtype)], axis=1
            )
        )
        lam_xy.append(np.repeat(col, 128, 1))
    rows = np.zeros((8, 256))
    for n, k in enumerate(lanes):
        if k < 0:
            continue
        if k < SPAN:
            rows[0, n], rows[2, n] = basis[0, k], basis[1, k]
        if k >= 7 * SPAN:
            rows[1, n], rows[3, n] = basis[17, k % SPAN], basis[16, k % SPAN]
        rows[4, n] = lam[k % SPAN]
    f32 = functools.partial(np.asarray, dtype=np.float32)
    return z_forward, np.stack(into), np.stack(out_of), z_back, f32(rows), f32(np.stack(lam_xy))


def dot(a, b):
    return lax.dot_general(a, b, NN, preferred_element_type=jnp.float32)


def halves(x):
    hi = x.astype(jnp.bfloat16)
    return hi, (x - hi.astype(jnp.float32)).astype(jnp.bfloat16)


def wide_halves(x):
    hi = x.astype(jnp.bfloat16).astype(jnp.float32)
    return hi, x - hi


def kernel(
    sizes, rhs_hbm, visc_hbm, reac_hbm, zf_hbm, into_hbm, outof_hbm, zb_hbm, row_hbm, lam_hbm,
    out_ref,
    rhs, first, resid, face, corner, zsend, zedge, rx, ry, rc, rz, re,
    part_hi, part_lo, end_hi, end_lo, ring, ring_end, inv, visc_plane, coef_plane,
    zf, into, outof, zb, row, lam, visc_ref, reac_ref, load_sem, send_sem, recv_sem, token,
):
    me = tuple(lax.axis_index(a) for a in ("gx", "gy", "gz"))

    def exists(d):
        ok = None
        for p, n, s in zip(me, sizes, d):
            if s:
                c = (p + s >= 0) & (p + s < n)
                ok = c if ok is None else ok & c
        return ok

    def peer(d):
        return tuple(p + s for p, s in zip(me, d))

    def minus(d):
        return tuple(-s for s in d)

    def greet(sem, dirs):
        count = jnp.int32(0)
        for d in dirs:
            ok = exists(d)
            count = count + ok.astype(jnp.int32)

            @pl.when(ok)
            def _(d=d):
                pl.semaphore_signal(sem, inc=1, device_id=peer(d), device_id_type=MESH)

        return count

    barrier = pltpu.get_barrier_semaphore()
    count = greet(barrier, FACES)

    loads = []
    pairs = [(rhs_hbm.at[c], rhs.at[c]) for c in range(3)]
    pairs += [(zf_hbm, zf), (visc_hbm, visc_ref), (reac_hbm, reac_ref), (row_hbm, row), (lam_hbm, lam), (into_hbm, into), (outof_hbm, outof), (zb_hbm, zb)]
    for k, (src, dst) in enumerate(pairs):
        loads.append(pltpu.make_async_copy(src, dst, load_sem.at[k]))
    for load in loads[:4]:
        load.start()

    def pieces(rnd, c, d):
        dx, dy, dz = d
        full = 0 if rnd == 0 else 1
        if dz == 0 and dy == 0:
            return face.at[rnd, c, pl.ds(X_LAST if dx > 0 else X_FIRST, 32), :], rx.at[rnd, int(dx > 0), c]
        if dz == 0 and dx == 0:
            return face.at[rnd, c, pl.ds(Y_LAST if dy > 0 else Y_FIRST, 16), :], ry.at[rnd, int(dy > 0), c]
        if dz == 0:
            k = 2 * int(dx > 0) + int(dy > 0)
            if rnd == 0:
                return corner.at[0, k], rc.at[0, k]
            return corner.at[full, k, c], rc.at[full, k, c]
        s = int(dz > 0)
        if dx == 0 and dy == 0:
            return zsend.at[rnd, s, c], rz.at[rnd, s, c]
        if rnd == 0:
            return zedge.at[0, s], re.at[0, s, slot(d)]
        return zedge.at[full, s, c], re.at[full, s, slot(d), c]

    def slot(d):
        return 3 * (d[0] + 1) + d[1] + 1

    copies = {}
    for rnd in range(3):
        for c in range(3):
            for d in DIRS if rnd == 2 or (rnd, c) == (0, 0) else FACES:
                k = len(copies)
                src, dst = pieces(rnd, c, d)
                copies[rnd, c, d] = pltpu.make_async_remote_copy(
                    src_ref=src, dst_ref=dst, send_sem=send_sem.at[k], recv_sem=recv_sem.at[k],
                    device_id=peer(d), device_id_type=MESH,
                )

    def send(rnd, c, ask):
        for (r, cc, d), copy in copies.items():
            if r == rnd and cc == c and ask(d):
                pl.when(exists(d))(copy.start)

    def arrive(rnd, c, ask=lambda d: True):
        for (r, cc, d), copy in copies.items():
            if r == rnd and cc == c and ask(d):
                pl.when(exists(minus(d)))(copy.wait_recv)

    def drain(rnd, which):
        for (r, c, d), copy in copies.items():
            if r == rnd and c in which:
                pl.when(exists(d))(copy.wait_send)

    flat = lambda d: d[2] == 0
    deep = lambda d: d[2] != 0

    lane = lax.broadcasted_iota(jnp.int32, (1, 128), 1)

    def by_element(ref, f, edge):
        v = jnp.zeros((1, 128), jnp.float32)
        for h in range(8):
            at = (lane >= edge * h) & (lane < edge * h + edge)
            v = jnp.where(at, ref[f, h], v)
        return v

    def fill_face(rnd, c, src):
        for k, y in enumerate((0, 15, 16, 31)):
            face[rnd, c, 16 * k : 16 * k + 8, :] = src[c, pl.ds(y, 8, stride=32), :]
            for x in range(8):
                at = 32 * (15 - x) + y
                face[rnd, c, 16 * k + 8 + x : 16 * k + 9 + x, :] = src[c, at : at + 1, :]
        face[rnd, c, X_FIRST : X_FIRST + 32, :] = src[c, 0:32]
        face[rnd, c, X_LAST : X_LAST + 32, :] = src[c, 480:512]

    def fill_corner(full, rnd, c):
        for k, at in enumerate((X_FIRST, X_FIRST + 31, X_LAST, X_LAST + 31)):
            corner[full, k, c] = face[rnd, c, at : at + 1, :]

    def z_forward(x):
        hi, lo = halves(x)
        return dot(jnp.concatenate([hi, lo, hi], axis=1), zf[...])

    def face_ends(rnd, c):
        hi, lo = halves(face[rnd, c])
        return dot(jnp.concatenate([hi, lo], axis=1), zf[:256, 128:])

    def gather_ends(ends, edge):
        total = ends[0]
        for k in range(1, 4):
            total = total + pltpu.roll(ends[k], k, 1)
        total = jnp.where(lane < HIGH + 4, total, pltpu.roll(edge, 16, 1))
        t = jnp.transpose(total)
        return t[LOW : LOW + 4], t[HIGH : HIGH + 4], t[LOW + 16 : LOW + 17], t[HIGH + 16 : HIGH + 17]

    def put_ends(rnd, c, low, high, edge_low, edge_high):
        for s, (planes, edge) in enumerate(((low, edge_low), (high, edge_high))):
            zsend[rnd, s, c, 0:4] = planes
            zsend[rnd, s, c, 4:5] = edge
            if rnd != 1:
                zedge[0 if rnd == 0 else 1, s, c] = edge

    def main_part(c, src):
        parts = []
        for f in range(2):
            near = [src[c, 32 * x + 16 * f : 32 * x + 16 * f + 16] for x in range(8)]
            far = [src[c, 32 * (15 - x) + 16 * f : 32 * (15 - x) + 16 * f + 16] for x in range(8)]
            parts += [n + m for n, m in zip(near, far)] + [n - m for n, m in zip(near, far)]
        m = z_forward(jnp.concatenate(parts, axis=0))
        ends = []
        for k in range(4):
            hi, lo = halves(m[128 * k : 128 * k + 128, :128])
            part_hi[c, k] = hi
            part_lo[c, k] = lo
            end = m[128 * k : 128 * k + 128, 128:]
            hi, lo = halves(jnp.where(lane < TAIL, end, 0.0))
            end_hi[c, k] = hi
            end_lo[c, k] = lo
            ends.append(end)
        return ends

    def ring_part(c, rnd, full):
        xm, xp = rx[rnd, 1, c], rx[rnd, 0, c]
        sums = (xm + xp, xm - xp)
        for p in range(2):
            fold = (lambda a, b: a + b) if p == 0 else (lambda a, b: a - b)
            ring[p, 0:16] = sums[p][0:16]
            ring[2 + p, 0:16] = sums[p][16:32]
            ym, yp = ry[rnd, 1, c], ry[rnd, 0, c]
            mid = face[rnd, c, Y_MID : Y_MID + 32]
            ring[p, 16:24] = fold(ym[0:8], ym[8:16])
            ring[p, 24:32] = fold(mid[16:24], mid[24:32])
            ring[2 + p, 16:24] = fold(mid[0:8], mid[8:16])
            ring[2 + p, 24:32] = fold(yp[0:8], yp[8:16])
            ring[p, 32:33] = fold(rc[full, 3, c], rc[full, 1, c])
            ring[p, 33:34] = sums[p][16:17]
            ring[2 + p, 32:33] = sums[p][15:16]
            ring[2 + p, 33:34] = fold(rc[full, 2, c], rc[full, 0, c])
        return z_forward(ring[...].reshape(4 * RING, 128))

    def ring_planes(c, full, rnd):
        rows = []
        for s in (1, 0):
            got = lambda dx, dy: re[full, s, slot((dx, dy)), c]
            own = rz[rnd, s, c, 4:5]
            t = jnp.where((lane >= 48) & (lane < 64), got(0, 1), own)
            t = jnp.where((lane >= 64) & (lane < 95), got(-1, 0), t)
            t = jnp.where(lane == 95, got(-1, 1), t)
            t = jnp.where((lane >= 96) & (lane < 127), got(1, 0), t)
            t = jnp.where(lane == 127, got(1, 1), t)
            rows += [t, t]
            t = jnp.where(lane < 16, got(0, -1), own)
            t = jnp.where(lane == 64, got(-1, -1), t)
            t = jnp.where((lane > 64) & (lane < 96), got(-1, 0), t)
            t = jnp.where(lane == 96, got(1, -1), t)
            t = jnp.where(lane > 96, got(1, 0), t)
            rows += [t, t]
        t = jnp.concatenate([jnp.zeros((LOW, 128), jnp.float32)] + rows + [jnp.zeros((120 - LOW, 128), jnp.float32)], axis=0)
        t = jnp.transpose(t)
        for p in range(2):
            fold = (lambda a, b: a + b) if p == 0 else (lambda a, b: a - b)
            ends = fold(t[96:128], t[64:96])
            ring_end[p, 0:16] = ends[0:16]
            ring_end[2 + p, 0:16] = ends[16:32]
            ring_end[p, 16:24] = fold(t[48:56], t[56:64])
            ring_end[p, 24:32] = fold(t[32:40], t[40:48])
            ring_end[2 + p, 16:24] = fold(t[16:24], t[24:32])
            ring_end[2 + p, 24:32] = fold(t[0:8], t[8:16])
            ring_end[p, 32:33] = ends[31:32]
            ring_end[p, 33:34] = ends[16:17]
            ring_end[2 + p, 32:33] = ends[15:16]
            ring_end[2 + p, 33:34] = ends[0:1]

    def solve(c, rnd, full, inner):
        around = ring_part(c, rnd, full)
        ring_planes(c, full, rnd)
        blank = lambda n: jnp.zeros((n, 128), jnp.float32)
        planes = [blank(LOW), rz[rnd, 1, c, 0:4], rz[rnd, 0, c, 0:4]]
        planes += [blank(8) if inner is None else inner, blank(112 - LOW)]
        plane_hi, plane_lo = halves(jnp.transpose(jnp.concatenate(planes, axis=0)))
        ms = []
        for k in range(4):
            hi = jnp.concatenate([part_hi[c, k], end_hi[c, k] + plane_hi], axis=1)
            lo = jnp.concatenate([part_lo[c, k], end_lo[c, k] + plane_lo], axis=1)
            r = around[RING * k : RING * k + RING]
            r = jnp.concatenate([r[:, :128], jnp.where(lane < TAIL, r[:, 128:], ring_end[k])], axis=1)
            rh, rl = wide_halves(r)
            r = jnp.concatenate([rh, rl, rh, jnp.zeros((8, 256), jnp.float32)], axis=0).astype(jnp.bfloat16)
            ms.append(dot(into[k % 2], jnp.concatenate([hi, lo, hi, r], axis=0))[:HALF])
        us = []
        for k in range(4):
            m = ms[k]
            column = lambda n: m[:, 128 + n + k : 129 + n + k]
            low = m[:, :128] + column(LOW) * row[0:1, :128]
            high = m[:, 128:] + column(HIGH) * row[1:2, 128:]
            if inner is not None:
                low = low + column(LOW + 8) * row[2:3, :128]
                high = high + column(HIGH + 8) * row[3:4, 128:]
            t = jnp.concatenate([low, high], axis=1) * inv[k]
            hi, lo = halves(t[:128])
            th, tl = wide_halves(t[128:])
            t = jnp.concatenate([th, tl, th, jnp.zeros((8, 256), jnp.float32)], axis=0).astype(jnp.bfloat16)
            data = jnp.concatenate([hi, lo, hi, t], axis=0)
            us.append(dot(outof[k % 2], data))
        outs = []
        for u in us:
            hi, lo = halves(u[:, :128])
            eh, el = wide_halves(u[:, 128:])
            end = jnp.where((lane >= SPAN) & (lane < 2 * SPAN), el, eh).astype(jnp.bfloat16)
            outs.append(jnp.concatenate([hi, lo, hi, end], axis=1))
        return jnp.concatenate(outs, axis=0)

    def unfold(x, put):
        for f in range(2):
            for i in range(8):
                s = x[256 * f + 16 * i : 256 * f + 16 * i + 16, :128]
                d = x[256 * f + 128 + 16 * i : 256 * f + 128 + 16 * i + 16, :128]
                put(32 * i + 16 * f, s + d)
                put(32 * (15 - i) + 16 * f, s - d)

    for c in range(3):
        loads[c].wait()
        fill_face(0, c, rhs)
        fill_corner(0, 0, c)
    pl.semaphore_wait(barrier, count)
    for c in range(3):
        send(0, c, lambda d: d in FACES and d[1] != 0)
    count = greet(token.at[0], [d for d in FACES if d[1] == 0])
    for c in range(3):
        send(0, c, lambda d: d in FACES and d[0] != 0)
    for load in loads[4:]:
        load.start()
    zsend[...] = jnp.zeros(zsend.shape, jnp.float32)
    for k in range(4):
        ring[k, 32:40] = jnp.zeros((8, 128), jnp.float32)
        ring_end[k, 32:40] = jnp.zeros((8, 128), jnp.float32)

    loads[3].wait()
    for c in range(3):
        ends = main_part(c, rhs)
        put_ends(0, c, *gather_ends(ends, face_ends(0, c)))
    pl.semaphore_wait(token.at[0], count)
    count = greet(token.at[1], [d for d in FACES if d[2] != 0])
    for c in range(3):
        send(0, c, lambda d: sum(map(abs, d)) == 2 and d[1] != 0)
    for c in range(3):
        send(0, c, lambda d: d[1] == 0 and d[2] != 0)
    pl.semaphore_wait(token.at[1], count)
    for c in range(3):
        send(0, c, lambda d: sum(map(abs, d)) == 3)

    for d in DIRS:
        @pl.when(jnp.logical_not(exists(minus(d))))
        def _(d=d):
            for rnd in range(3):
                for c in range(3):
                    if d in FACES or rnd == 2 or (rnd, c) == (0, 0):
                        dst = pieces(rnd, c, d)[1]
                        dst[...] = jnp.zeros(dst.shape, jnp.float32)

    for k in range(4, 11):
        loads[k].wait()

    for f in range(2):
        for t in range(2):
            part = slice(128 * t, 128 * t + 128)
            if t == 0:
                v, r = by_element(visc_ref, f, SPAN), by_element(reac_ref, f, SPAN)
                v = jnp.where(lane >= 7 * SPAN, visc_ref[f, 7], v)
                r = jnp.where(lane >= 7 * SPAN, reac_ref[f, 7], r)
            else:
                v, r = jnp.full((1, 128), visc_ref[f, 7]), jnp.full((1, 128), reac_ref[f, 7])
            for p in range(2):
                inv[2 * f + p, :, part] = 1.0 / (v * (lam[p] + row[4:5, part]) + r)
        v, r = by_element(visc_ref, f, EDGE), by_element(reac_ref, f, EDGE)
        visc_plane[16 * f : 16 * f + 16] = jnp.broadcast_to(v, (16, 128))
        coef_plane[16 * f : 16 * f + 16] = jnp.broadcast_to(r + 6.0 * v, (16, 128))

    part_row = lax.broadcasted_iota(jnp.int32, (4, 128), 0)
    upper = ((lane >= 32) & (lane < 64)) | ((lane >= 80) & (lane < 96)) | (lane >= 112)
    plane_visc = [jnp.where(part_row < 2, visc_ref[0, h], visc_ref[1, h]) for h in (0, 7)]
    edge_visc = [jnp.where(upper, visc_ref[1, h], visc_ref[0, h]) for h in (0, 7)]

    for c in range(3):
        arrive(0, c)
        lhs = solve(c, 0, 0, None)
        x = dot(lhs, zb[...])

        def put_first(at, v, c=c):
            first[c, at : at + 16] = v

        unfold(x, put_first)
        fill_face(1, c, first)
        send(1, c, flat)
        ends = [x[128 * k : 128 * k + 128, 128:] for k in range(4)]
        put_ends(1, c, *gather_ends(ends, face_ends(1, c)))
        send(1, c, deep)

    y_index = lax.broadcasted_iota(jnp.int32, (32, 128), 0)
    inner = []
    for c in range(3):
        arrive(1, c)
        for x in range(16):
            v = first[c, 32 * x : 32 * x + 32]
            beside = rx[1, 1, c] if x == 0 else first[c, 32 * x - 32 : 32 * x]
            beside = beside + (rx[1, 0, c] if x == 15 else first[c, 32 * x + 32 : 32 * x + 64])
            at = x if x < 8 else 23 - x
            ylo, yhi = ry[1, 1, c, at : at + 1], ry[1, 0, c, at : at + 1]
            beside = beside + jnp.where(y_index == 0, ylo, pltpu.roll(v, 1, 0))
            beside = beside + jnp.where(y_index == 31, yhi, pltpu.roll(v, 31, 0))
            beside = beside + jnp.where(lane == 0, 0.0, pltpu.roll(v, 1, 1))
            beside = beside + jnp.where(lane == 127, 0.0, pltpu.roll(v, 127, 1))
            resid[c, 32 * x : 32 * x + 32] = (
                rhs[c, 32 * x : 32 * x + 32] - coef_plane[...] * v + visc_plane[...] * beside
            )
        fill_face(2, c, resid)
        planes = [plane_visc[s] * rz[1, 1 - s, c, 0:4] for s in range(2)]
        edge = [edge_visc[s] * rz[1, 1 - s, c, 4:5] for s in range(2)]
        inner.append(jnp.concatenate(planes, axis=0))
        face_low_high = face_ends(2, c)
        add = jnp.transpose(
            jnp.concatenate([edge[0], jnp.zeros((126, 128), jnp.float32), edge[1]], axis=0)
        )
        face[2, c] = face[2, c] + add
        fill_corner(1, 2, c)
        send(2, c, flat)
        ends = main_part(c, resid)
        low, high, edge_low, edge_high = gather_ends(ends, face_low_high)
        put_ends(2, c, low + planes[0], high + planes[1], edge_low + edge[0], edge_high + edge[1])
        send(2, c, deep)

    drain(0, (0, 1, 2))
    drain(1, (0, 1, 2))
    for c in range(3):
        if c:
            drain(2, (c - 1,))
        arrive(2, c)
        lhs = solve(c, 2, 1, inner[c])
        x = dot(lhs, zb[:, :128])

        def put_last(at, v, c=c):
            out_ref[c, at : at + 16] = first[c, at : at + 16] + v

        unfold(x, put_last)

    drain(2, (2,))


def shards(sizes, rhs, viscous, reaction):
    f32, bf16 = jnp.float32, jnp.bfloat16
    consts = constants()
    any_space = pl.BlockSpec(memory_space=pl.ANY)
    vmem = pl.BlockSpec(memory_space=pltpu.VMEM)
    copies = 3 * (2 * len(DIRS) + len(FACES))
    scratch = [
        pltpu.VMEM((3, 512, 128), f32),
        pltpu.VMEM((3, 512, 128), f32),
        pltpu.VMEM((3, 512, 128), f32),
        pltpu.VMEM((3, 3, 128, 128), f32),
        pltpu.VMEM((2, 4, 3, 1, 128), f32),
        pltpu.VMEM((3, 2, 3, 8, 128), f32),
        pltpu.VMEM((2, 2, 3, 1, 128), f32),
        pltpu.VMEM((3, 2, 3, 32, 128), f32),
        pltpu.VMEM((3, 2, 3, 16, 128), f32),
        pltpu.VMEM((2, 4, 3, 1, 128), f32),
        pltpu.VMEM((3, 2, 3, 8, 128), f32),
        pltpu.VMEM((2, 2, 9, 3, 1, 128), f32),
        pltpu.VMEM((3, 4, 128, 128), bf16),
        pltpu.VMEM((3, 4, 128, 128), bf16),
        pltpu.VMEM((3, 4, 128, 128), bf16),
        pltpu.VMEM((3, 4, 128, 128), bf16),
        pltpu.VMEM((4, RING, 128), f32),
        pltpu.VMEM((4, RING, 128), f32),
        pltpu.VMEM((4, HALF, 256), f32),
        pltpu.VMEM((32, 128), f32),
        pltpu.VMEM((32, 128), f32),
    ]
    scratch += [pltpu.VMEM(t.shape, t.dtype) for t in consts]
    scratch += [
        pltpu.SMEM((2, 8), f32),
        pltpu.SMEM((2, 8), f32),
        pltpu.SemaphoreType.DMA((11,)),
        pltpu.SemaphoreType.DMA((copies,)),
        pltpu.SemaphoreType.DMA((copies,)),
        pltpu.SemaphoreType.REGULAR((2,)),
    ]
    operands = (rhs.reshape(3, 512, 128), viscous.reshape(2, 8), reaction.reshape(2, 8), *consts)
    out = pl.pallas_call(
        functools.partial(kernel, sizes),
        out_shape=jax.ShapeDtypeStruct((3, 512, 128), f32),
        in_specs=[any_space] * len(operands),
        out_specs=vmem,
        scratch_shapes=scratch,
        compiler_params=pltpu.CompilerParams(
            collective_id=0, has_side_effects=True, vmem_limit_bytes=40 * 2**20
        ),
    )(*[pltpu.with_memory_space_constraint(jnp.asarray(a), pltpu.HBM) for a in operands])
    return out.reshape(rhs.shape)


def solution(mesh):
    sizes = tuple(mesh.shape[a] for a in ("gx", "gy", "gz"))
    placed = (P(None, "gx", "gy", "gz"), P("gx", "gy", "gz"), P("gx", "gy", "gz"))
    return jax.shard_map(
        functools.partial(shards, sizes),
        mesh=mesh,
        in_specs=placed,
        out_specs=P(None, "gx", "gy", "gz"),
        check_vma=False,
    )
```

```python
import functools

import jax
import jax.numpy as jnp
import numpy as np
from jax import lax
from jax.experimental import pallas as pl
from jax.experimental.pallas import tpu as pltpu
from jax.sharding import PartitionSpec as P

EDGE = 16
SPAN = EDGE + 2
HALF = 168
RING = 40
TAIL = 3 * SPAN
LOW, HIGH = 64, 68
MESH = pl.DeviceIdType.MESH
NN = (((1,), (0,)), ((), ()))
DIRS = [
    (dx, dy, dz)
    for dz in (0, -1, 1)
    for dy in (0, -1, 1)
    for dx in (0, -1, 1)
    if (dx, dy, dz) != (0, 0, 0)
]
FACES = [d for d in DIRS if sum(map(abs, d)) == 1]
Y_FIRST, Y_MID, Y_LAST, X_FIRST, X_LAST = 0, 16, 48, 64, 96


def table_halves(x):
    x = x.astype(np.float32)
    hi = x.astype(jnp.bfloat16)
    return hi, (x - hi.astype(np.float32)).astype(jnp.bfloat16)


def constants():
    i = np.arange(SPAN)
    basis = np.sqrt(2.0 / (SPAN + 1)) * np.sin(np.pi * np.outer(i + 1, i + 1) / (SPAN + 1))
    lam = 2.0 - 2.0 * np.cos(np.pi * (i + 1) / (SPAN + 1))
    lanes = np.concatenate([np.arange(126), [-1, -1], np.tile(np.arange(126, 144), 3)])
    forward = np.zeros((128, 256))
    back = np.zeros((144, 128))
    for h in range(8):
        for z in range(128):
            w = z - EDGE * h + 1
            if 0 <= w < SPAN:
                for n, k in enumerate(lanes):
                    if k >= 0 and k // SPAN == h:
                        forward[z, n] = basis[w, k % SPAN]
            if 1 <= w <= EDGE:
                back[h * SPAN : (h + 1) * SPAN, z] = basis[w]
    forward[0, 128 + LOW] = 1.0
    forward[127, 128 + HIGH] = 1.0
    wide = np.zeros((144, 256))
    wide[:, :128] = back
    wide[:, 128 + LOW] = 2.0 * back[:, 0]
    wide[:, 128 + HIGH] = 2.0 * back[:, 127]
    fh, fl = table_halves(forward)
    bh, bl = table_halves(wide)
    z_forward = np.concatenate([fh, fh, fl], axis=0)
    pad = lambda n: np.zeros((n, 256), bh.dtype)
    z_back = np.concatenate(
        [bh[:126], pad(2), bh[:126], pad(2), bl[:126], pad(2), bh[126:], bh[126:], bl[126:], pad(74)], axis=0
    )
    into, out_of, lam_xy = [], [], []
    for parity in range(2):
        mode = np.arange(162)
        a, b = 2 * (mode // SPAN) + parity, mode % SPAN
        point = lambda x, y: basis[x, a] * basis[y, b]
        main = np.zeros((176, 128))
        for x in range(8):
            for y in range(16):
                main[:162, 16 * x + y] = point(x + 1, y + 1)
        ring = np.zeros((176, RING))
        for y in range(16):
            ring[:162, y] = point(0, y + 1)
        for x in range(8):
            ring[:162, 16 + x] = point(x + 1, 0)
            ring[:162, 24 + x] = point(x + 1, 17)
        ring[:162, 32], ring[:162, 33] = point(0, 0), point(0, 17)
        mh, ml = table_halves(main)
        rh, rl = table_halves(ring)
        into.append(np.concatenate([mh, mh, ml, rh, rh, rl, np.zeros((176, 8), mh.dtype)], axis=1))
        col = np.zeros((HALF, 1))
        col[:162, 0] = lam[a] + lam[b]
        th, tl = mh[:HALF].T, ml[:HALF].T
        a, b = slice(0, 128), slice(128, HALF)
        out_of.append(
            np.concatenate(
                [th[:, a], th[:, a], tl[:, a], th[:, b], th[:, b], tl[:, b], np.zeros((128, 8), mh.dtype)], axis=1
            )
        )
        lam_xy.append(np.repeat(col, 128, 1))
    rows = np.zeros((8, 256))
    for n, k in enumerate(lanes):
        if k < 0:
            continue
        if k < SPAN:
            rows[0, n], rows[2, n] = basis[0, k], basis[1, k]
        if k >= 7 * SPAN:
            rows[1, n], rows[3, n] = basis[17, k % SPAN], basis[16, k % SPAN]
        rows[4, n] = lam[k % SPAN]
    f32 = functools.partial(np.asarray, dtype=np.float32)
    return z_forward, np.stack(into), np.stack(out_of), z_back, f32(rows), f32(np.stack(lam_xy))


def dot(a, b):
    return lax.dot_general(a, b, NN, preferred_element_type=jnp.float32)


def halves(x):
    hi = x.astype(jnp.bfloat16)
    return hi, (x - hi.astype(jnp.float32)).astype(jnp.bfloat16)


def wide_halves(x):
    hi = x.astype(jnp.bfloat16).astype(jnp.float32)
    return hi, x - hi


def kernel(
    sizes, rhs_hbm, visc_hbm, reac_hbm, zf_hbm, into_hbm, outof_hbm, zb_hbm, row_hbm, lam_hbm,
    out_ref,
    rhs, first, resid, face, corner, zsend, zedge, rx, ry, rc, rz, re,
    part_hi, part_lo, end_hi, end_lo, ring, ring_end, inv, visc_plane, coef_plane,
    zf, into, outof, zb, row, lam, visc_ref, reac_ref, load_sem, send_sem, recv_sem, token,
):
    me = tuple(lax.axis_index(a) for a in ("gx", "gy", "gz"))

    def exists(d):
        ok = None
        for p, n, s in zip(me, sizes, d):
            if s:
                c = (p + s >= 0) & (p + s < n)
                ok = c if ok is None else ok & c
        return ok

    def peer(d):
        return tuple(p + s for p, s in zip(me, d))

    def minus(d):
        return tuple(-s for s in d)

    def greet(sem, dirs):
        count = jnp.int32(0)
        for d in dirs:
            ok = exists(d)
            count = count + ok.astype(jnp.int32)

            @pl.when(ok)
            def _(d=d):
                pl.semaphore_signal(sem, inc=1, device_id=peer(d), device_id_type=MESH)

        return count

    barrier = pltpu.get_barrier_semaphore()
    count = greet(barrier, FACES)

    loads = []
    pairs = [(rhs_hbm.at[c], rhs.at[c]) for c in range(3)]
    pairs += [(zf_hbm, zf), (visc_hbm, visc_ref), (reac_hbm, reac_ref), (row_hbm, row), (lam_hbm, lam), (into_hbm, into), (outof_hbm, outof), (zb_hbm, zb)]
    for k, (src, dst) in enumerate(pairs):
        loads.append(pltpu.make_async_copy(src, dst, load_sem.at[k]))
    for load in loads[:4]:
        load.start()

    def pieces(rnd, c, d):
        dx, dy, dz = d
        full = 0 if rnd == 0 else 1
        if dz == 0 and dy == 0:
            return face.at[rnd, c, pl.ds(X_LAST if dx > 0 else X_FIRST, 32), :], rx.at[rnd, int(dx > 0), c]
        if dz == 0 and dx == 0:
            return face.at[rnd, c, pl.ds(Y_LAST if dy > 0 else Y_FIRST, 16), :], ry.at[rnd, int(dy > 0), c]
        if dz == 0:
            k = 2 * int(dx > 0) + int(dy > 0)
            if rnd == 0:
                return corner.at[0, k], rc.at[0, k]
            return corner.at[full, k, c], rc.at[full, k, c]
        s = int(dz > 0)
        if dx == 0 and dy == 0:
            return zsend.at[rnd, s, c], rz.at[rnd, s, c]
        if rnd == 0:
            return zedge.at[0, s], re.at[0, s, slot(d)]
        return zedge.at[full, s, c], re.at[full, s, slot(d), c]

    def slot(d):
        return 3 * (d[0] + 1) + d[1] + 1

    copies = {}
    for rnd in range(3):
        for c in range(3):
            for d in DIRS if rnd == 2 or (rnd, c) == (0, 0) else FACES:
                k = len(copies)
                src, dst = pieces(rnd, c, d)
                copies[rnd, c, d] = pltpu.make_async_remote_copy(
                    src_ref=src, dst_ref=dst, send_sem=send_sem.at[k], recv_sem=recv_sem.at[k],
                    device_id=peer(d), device_id_type=MESH,
                )

    def send(rnd, c, ask):
        for (r, cc, d), copy in sorted(copies.items(), key=lambda item: -abs(item[0][2][1])):
            if r == rnd and cc == c and ask(d):
                pl.when(exists(d))(copy.start)

    def arrive(rnd, c, ask=lambda d: True):
        for (r, cc, d), copy in copies.items():
            if r == rnd and cc == c and ask(d):
                pl.when(exists(minus(d)))(copy.wait_recv)

    def drain(rnd, which):
        for (r, c, d), copy in copies.items():
            if r == rnd and c in which:
                pl.when(exists(d))(copy.wait_send)

    flat = lambda d: d[2] == 0
    deep = lambda d: d[2] != 0

    lane = lax.broadcasted_iota(jnp.int32, (1, 128), 1)

    def by_element(ref, f, edge):
        v = jnp.zeros((1, 128), jnp.float32)
        for h in range(8):
            at = (lane >= edge * h) & (lane < edge * h + edge)
            v = jnp.where(at, ref[f, h], v)
        return v

    def fill_face(rnd, c, src):
        for k, y in enumerate((0, 15, 16, 31)):
            face[rnd, c, 16 * k : 16 * k + 8, :] = src[c, pl.ds(y, 8, stride=32), :]
            for x in range(8):
                at = 32 * (15 - x) + y
                face[rnd, c, 16 * k + 8 + x : 16 * k + 9 + x, :] = src[c, at : at + 1, :]
        face[rnd, c, X_FIRST : X_FIRST + 32, :] = src[c, 0:32]
        face[rnd, c, X_LAST : X_LAST + 32, :] = src[c, 480:512]

    def fill_corner(full, rnd, c):
        for k, at in enumerate((X_FIRST, X_FIRST + 31, X_LAST, X_LAST + 31)):
            corner[full, k, c] = face[rnd, c, at : at + 1, :]

    def z_forward(x):
        hi, lo = halves(x)
        return dot(jnp.concatenate([hi, lo, hi], axis=1), zf[...])

    def face_ends(rnd, c):
        hi, lo = halves(face[rnd, c])
        return dot(jnp.concatenate([hi, lo], axis=1), zf[:256, 128:])

    def gather_ends(ends, edge):
        total = ends[0]
        for k in range(1, 4):
            total = total + pltpu.roll(ends[k], k, 1)
        total = jnp.where(lane < HIGH + 4, total, pltpu.roll(edge, 16, 1))
        t = jnp.transpose(total)
        return t[LOW : LOW + 4], t[HIGH : HIGH + 4], t[LOW + 16 : LOW + 17], t[HIGH + 16 : HIGH + 17]

    def put_ends(rnd, c, low, high, edge_low, edge_high):
        for s, (planes, edge) in enumerate(((low, edge_low), (high, edge_high))):
            zsend[rnd, s, c, 0:4] = planes
            zsend[rnd, s, c, 4:5] = edge
            if rnd != 1:
                zedge[0 if rnd == 0 else 1, s, c] = edge

    def main_part(c, src):
        parts = []
        for f in range(2):
            near = [src[c, 32 * x + 16 * f : 32 * x + 16 * f + 16] for x in range(8)]
            far = [src[c, 32 * (15 - x) + 16 * f : 32 * (15 - x) + 16 * f + 16] for x in range(8)]
            parts += [n + m for n, m in zip(near, far)] + [n - m for n, m in zip(near, far)]
        m = z_forward(jnp.concatenate(parts, axis=0))
        ends = []
        for k in range(4):
            hi, lo = halves(m[128 * k : 128 * k + 128, :128])
            part_hi[c, k] = hi
            part_lo[c, k] = lo
            end = m[128 * k : 128 * k + 128, 128:]
            hi, lo = halves(jnp.where(lane < TAIL, end, 0.0))
            end_hi[c, k] = hi
            end_lo[c, k] = lo
            ends.append(end)
        return ends

    def ring_part(c, rnd, full):
        xm, xp = rx[rnd, 1, c], rx[rnd, 0, c]
        sums = (xm + xp, xm - xp)
        for p in range(2):
            fold = (lambda a, b: a + b) if p == 0 else (lambda a, b: a - b)
            ring[p, 0:16] = sums[p][0:16]
            ring[2 + p, 0:16] = sums[p][16:32]
            ym, yp = ry[rnd, 1, c], ry[rnd, 0, c]
            mid = face[rnd, c, Y_MID : Y_MID + 32]
            ring[p, 16:24] = fold(ym[0:8], ym[8:16])
            ring[p, 24:32] = fold(mid[16:24], mid[24:32])
            ring[2 + p, 16:24] = fold(mid[0:8], mid[8:16])
            ring[2 + p, 24:32] = fold(yp[0:8], yp[8:16])
            ring[p, 32:33] = fold(rc[full, 3, c], rc[full, 1, c])
            ring[p, 33:34] = sums[p][16:17]
            ring[2 + p, 32:33] = sums[p][15:16]
            ring[2 + p, 33:34] = fold(rc[full, 2, c], rc[full, 0, c])
        return z_forward(ring[...].reshape(4 * RING, 128))

    def ring_planes(c, full, rnd):
        rows = []
        for s in (1, 0):
            got = lambda dx, dy: re[full, s, slot((dx, dy)), c]
            own = rz[rnd, s, c, 4:5]
            t = jnp.where((lane >= 48) & (lane < 64), got(0, 1), own)
            t = jnp.where((lane >= 64) & (lane < 95), got(-1, 0), t)
            t = jnp.where(lane == 95, got(-1, 1), t)
            t = jnp.where((lane >= 96) & (lane < 127), got(1, 0), t)
            t = jnp.where(lane == 127, got(1, 1), t)
            rows += [t, t]
            t = jnp.where(lane < 16, got(0, -1), own)
            t = jnp.where(lane == 64, got(-1, -1), t)
            t = jnp.where((lane > 64) & (lane < 96), got(-1, 0), t)
            t = jnp.where(lane == 96, got(1, -1), t)
            t = jnp.where(lane > 96, got(1, 0), t)
            rows += [t, t]
        t = jnp.concatenate([jnp.zeros((LOW, 128), jnp.float32)] + rows + [jnp.zeros((120 - LOW, 128), jnp.float32)], axis=0)
        t = jnp.transpose(t)
        for p in range(2):
            fold = (lambda a, b: a + b) if p == 0 else (lambda a, b: a - b)
            ends = fold(t[96:128], t[64:96])
            ring_end[p, 0:16] = ends[0:16]
            ring_end[2 + p, 0:16] = ends[16:32]
            ring_end[p, 16:24] = fold(t[48:56], t[56:64])
            ring_end[p, 24:32] = fold(t[32:40], t[40:48])
            ring_end[2 + p, 16:24] = fold(t[16:24], t[24:32])
            ring_end[2 + p, 24:32] = fold(t[0:8], t[8:16])
            ring_end[p, 32:33] = ends[31:32]
            ring_end[p, 33:34] = ends[16:17]
            ring_end[2 + p, 32:33] = ends[15:16]
            ring_end[2 + p, 33:34] = ends[0:1]

    def solve(c, rnd, full, inner):
        around = ring_part(c, rnd, full)
        ring_planes(c, full, rnd)
        blank = lambda n: jnp.zeros((n, 128), jnp.float32)
        planes = [blank(LOW), rz[rnd, 1, c, 0:4], rz[rnd, 0, c, 0:4]]
        planes += [blank(8) if inner is None else inner, blank(112 - LOW)]
        plane_hi, plane_lo = halves(jnp.transpose(jnp.concatenate(planes, axis=0)))
        ms = []
        for k in range(4):
            hi = jnp.concatenate([part_hi[c, k], end_hi[c, k] + plane_hi], axis=1)
            lo = jnp.concatenate([part_lo[c, k], end_lo[c, k] + plane_lo], axis=1)
            r = around[RING * k : RING * k + RING]
            r = jnp.concatenate([r[:, :128], jnp.where(lane < TAIL, r[:, 128:], ring_end[k])], axis=1)
            rh, rl = wide_halves(r)
            r = jnp.concatenate([rh, rl, rh, jnp.zeros((8, 256), jnp.float32)], axis=0).astype(jnp.bfloat16)
            ms.append(dot(into[k % 2], jnp.concatenate([hi, lo, hi, r], axis=0))[:HALF])
        us = []
        for k in range(4):
            m = ms[k]
            column = lambda n: m[:, 128 + n + k : 129 + n + k]
            low = m[:, :128] + column(LOW) * row[0:1, :128]
            high = m[:, 128:] + column(HIGH) * row[1:2, 128:]
            if inner is not None:
                low = low + column(LOW + 8) * row[2:3, :128]
                high = high + column(HIGH + 8) * row[3:4, 128:]
            t = jnp.concatenate([low, high], axis=1) * inv[k]
            hi, lo = halves(t[:128])
            th, tl = wide_halves(t[128:])
            t = jnp.concatenate([th, tl, th, jnp.zeros((8, 256), jnp.float32)], axis=0).astype(jnp.bfloat16)
            data = jnp.concatenate([hi, lo, hi, t], axis=0)
            us.append(dot(outof[k % 2], data))
        outs = []
        for u in us:
            hi, lo = halves(u[:, :128])
            eh, el = wide_halves(u[:, 128:])
            end = jnp.where((lane >= SPAN) & (lane < 2 * SPAN), el, eh).astype(jnp.bfloat16)
            outs.append(jnp.concatenate([hi, lo, hi, end], axis=1))
        return jnp.concatenate(outs, axis=0)

    def unfold(x, put):
        for f in range(2):
            for i in range(8):
                s = x[256 * f + 16 * i : 256 * f + 16 * i + 16, :128]
                d = x[256 * f + 128 + 16 * i : 256 * f + 128 + 16 * i + 16, :128]
                put(32 * i + 16 * f, s + d)
                put(32 * (15 - i) + 16 * f, s - d)

    for c in range(3):
        loads[c].wait()
        fill_face(0, c, rhs)
        fill_corner(0, 0, c)
    pl.semaphore_wait(barrier, count)
    for c in range(3):
        send(0, c, lambda d: d in FACES and d[1] != 0)
    count = greet(token.at[0], [d for d in FACES if d[1] == 0])
    for c in range(3):
        send(0, c, lambda d: d in FACES and d[0] != 0)
    for load in loads[4:]:
        load.start()
    zsend[...] = jnp.zeros(zsend.shape, jnp.float32)
    for k in range(4):
        ring[k, 32:40] = jnp.zeros((8, 128), jnp.float32)
        ring_end[k, 32:40] = jnp.zeros((8, 128), jnp.float32)

    loads[3].wait()
    for c in range(3):
        ends = main_part(c, rhs)
        put_ends(0, c, *gather_ends(ends, face_ends(0, c)))
    pl.semaphore_wait(token.at[0], count)
    count = greet(token.at[1], [d for d in FACES if d[2] != 0])
    for c in range(3):
        send(0, c, lambda d: sum(map(abs, d)) == 2 and d[1] != 0)
    for c in range(3):
        send(0, c, lambda d: d[1] == 0 and d[2] != 0)
    pl.semaphore_wait(token.at[1], count)
    for c in range(3):
        send(0, c, lambda d: sum(map(abs, d)) == 3)

    for d in DIRS:
        @pl.when(jnp.logical_not(exists(minus(d))))
        def _(d=d):
            for rnd in range(3):
                for c in range(3):
                    if d in FACES or rnd == 2 or (rnd, c) == (0, 0):
                        dst = pieces(rnd, c, d)[1]
                        dst[...] = jnp.zeros(dst.shape, jnp.float32)

    for k in range(4, 11):
        loads[k].wait()

    for f in range(2):
        for t in range(2):
            part = slice(128 * t, 128 * t + 128)
            if t == 0:
                v, r = by_element(visc_ref, f, SPAN), by_element(reac_ref, f, SPAN)
                v = jnp.where(lane >= 7 * SPAN, visc_ref[f, 7], v)
                r = jnp.where(lane >= 7 * SPAN, reac_ref[f, 7], r)
            else:
                v, r = jnp.full((1, 128), visc_ref[f, 7]), jnp.full((1, 128), reac_ref[f, 7])
            for p in range(2):
                inv[2 * f + p, :, part] = 1.0 / (v * (lam[p] + row[4:5, part]) + r)
        v, r = by_element(visc_ref, f, EDGE), by_element(reac_ref, f, EDGE)
        visc_plane[16 * f : 16 * f + 16] = jnp.broadcast_to(v, (16, 128))
        coef_plane[16 * f : 16 * f + 16] = jnp.broadcast_to(r + 6.0 * v, (16, 128))

    part_row = lax.broadcasted_iota(jnp.int32, (4, 128), 0)
    upper = ((lane >= 32) & (lane < 64)) | ((lane >= 80) & (lane < 96)) | (lane >= 112)
    plane_visc = [jnp.where(part_row < 2, visc_ref[0, h], visc_ref[1, h]) for h in (0, 7)]
    edge_visc = [jnp.where(upper, visc_ref[1, h], visc_ref[0, h]) for h in (0, 7)]

    for c in range(3):
        arrive(0, c)
        lhs = solve(c, 0, 0, None)
        x = dot(lhs, zb[...])

        def put_first(at, v, c=c):
            first[c, at : at + 16] = v

        unfold(x, put_first)
        fill_face(1, c, first)
        send(1, c, flat)
        ends = [x[128 * k : 128 * k + 128, 128:] for k in range(4)]
        put_ends(1, c, *gather_ends(ends, face_ends(1, c)))
        send(1, c, deep)

    y_index = lax.broadcasted_iota(jnp.int32, (32, 128), 0)
    inner = []
    for c in range(3):
        arrive(1, c)
        for x in range(16):
            v = first[c, 32 * x : 32 * x + 32]
            beside = rx[1, 1, c] if x == 0 else first[c, 32 * x - 32 : 32 * x]
            beside = beside + (rx[1, 0, c] if x == 15 else first[c, 32 * x + 32 : 32 * x + 64])
            at = x if x < 8 else 23 - x
            ylo, yhi = ry[1, 1, c, at : at + 1], ry[1, 0, c, at : at + 1]
            beside = beside + jnp.where(y_index == 0, ylo, pltpu.roll(v, 1, 0))
            beside = beside + jnp.where(y_index == 31, yhi, pltpu.roll(v, 31, 0))
            beside = beside + jnp.where(lane == 0, 0.0, pltpu.roll(v, 1, 1))
            beside = beside + jnp.where(lane == 127, 0.0, pltpu.roll(v, 127, 1))
            resid[c, 32 * x : 32 * x + 32] = (
                rhs[c, 32 * x : 32 * x + 32] - coef_plane[...] * v + visc_plane[...] * beside
            )
        fill_face(2, c, resid)
        planes = [plane_visc[s] * rz[1, 1 - s, c, 0:4] for s in range(2)]
        edge = [edge_visc[s] * rz[1, 1 - s, c, 4:5] for s in range(2)]
        inner.append(jnp.concatenate(planes, axis=0))
        face_low_high = face_ends(2, c)
        add = jnp.transpose(
            jnp.concatenate([edge[0], jnp.zeros((126, 128), jnp.float32), edge[1]], axis=0)
        )
        face[2, c] = face[2, c] + add
        fill_corner(1, 2, c)
        send(2, c, flat)
        ends = main_part(c, resid)
        low, high, edge_low, edge_high = gather_ends(ends, face_low_high)
        put_ends(2, c, low + planes[0], high + planes[1], edge_low + edge[0], edge_high + edge[1])
        send(2, c, deep)

    drain(0, (0, 1, 2))
    drain(1, (0, 1, 2))
    for c in range(3):
        if c:
            drain(2, (c - 1,))
        arrive(2, c)
        lhs = solve(c, 2, 1, inner[c])
        x = dot(lhs, zb[:, :128])

        def put_last(at, v, c=c):
            out_ref[c, at : at + 16] = first[c, at : at + 16] + v

        unfold(x, put_last)

    drain(2, (2,))


def shards(sizes, rhs, viscous, reaction):
    f32, bf16 = jnp.float32, jnp.bfloat16
    consts = constants()
    any_space = pl.BlockSpec(memory_space=pl.ANY)
    vmem = pl.BlockSpec(memory_space=pltpu.VMEM)
    copies = 3 * (2 * len(DIRS) + len(FACES))
    scratch = [
        pltpu.VMEM((3, 512, 128), f32),
        pltpu.VMEM((3, 512, 128), f32),
        pltpu.VMEM((3, 512, 128), f32),
        pltpu.VMEM((3, 3, 128, 128), f32),
        pltpu.VMEM((2, 4, 3, 1, 128), f32),
        pltpu.VMEM((3, 2, 3, 8, 128), f32),
        pltpu.VMEM((2, 2, 3, 1, 128), f32),
        pltpu.VMEM((3, 2, 3, 32, 128), f32),
        pltpu.VMEM((3, 2, 3, 16, 128), f32),
        pltpu.VMEM((2, 4, 3, 1, 128), f32),
        pltpu.VMEM((3, 2, 3, 8, 128), f32),
        pltpu.VMEM((2, 2, 9, 3, 1, 128), f32),
        pltpu.VMEM((3, 4, 128, 128), bf16),
        pltpu.VMEM((3, 4, 128, 128), bf16),
        pltpu.VMEM((3, 4, 128, 128), bf16),
        pltpu.VMEM((3, 4, 128, 128), bf16),
        pltpu.VMEM((4, RING, 128), f32),
        pltpu.VMEM((4, RING, 128), f32),
        pltpu.VMEM((4, HALF, 256), f32),
        pltpu.VMEM((32, 128), f32),
        pltpu.VMEM((32, 128), f32),
    ]
    scratch += [pltpu.VMEM(t.shape, t.dtype) for t in consts]
    scratch += [
        pltpu.SMEM((2, 8), f32),
        pltpu.SMEM((2, 8), f32),
        pltpu.SemaphoreType.DMA((11,)),
        pltpu.SemaphoreType.DMA((copies,)),
        pltpu.SemaphoreType.DMA((copies,)),
        pltpu.SemaphoreType.REGULAR((2,)),
    ]
    operands = (rhs.reshape(3, 512, 128), viscous.reshape(2, 8), reaction.reshape(2, 8), *consts)
    out = pl.pallas_call(
        functools.partial(kernel, sizes),
        out_shape=jax.ShapeDtypeStruct((3, 512, 128), f32),
        in_specs=[any_space] * len(operands),
        out_specs=vmem,
        scratch_shapes=scratch,
        compiler_params=pltpu.CompilerParams(
            collective_id=0, has_side_effects=True, vmem_limit_bytes=40 * 2**20
        ),
    )(*[pltpu.with_memory_space_constraint(jnp.asarray(a), pltpu.HBM) for a in operands])
    return out.reshape(rhs.shape)


def solution(mesh):
    sizes = tuple(mesh.shape[a] for a in ("gx", "gy", "gz"))
    placed = (P(None, "gx", "gy", "gz"), P("gx", "gy", "gz"), P("gx", "gy", "gz"))
    return jax.shard_map(
        functools.partial(shards, sizes),
        mesh=mesh,
        in_specs=placed,
        out_specs=P(None, "gx", "gy", "gz"),
        check_vma=False,
    )
```
